128 devices in a mesh: data: 1, col: 64 (over z, y, x), row: 2 (over core).
Axes of the slice: x: 4, y: 4, z: 4, core: 2. Of those that a mesh axis runs over, the one named last changes fastest.
Arguments:
- pair_rep: bfloat16 [1024, 1024, 64], P(('data', 'row'), 'col')
- res_mask: int32 [1024], P('data')
- ln_gamma: float32 [64], replicated
- ln_beta: float32 [64], replicated
- w_q: bfloat16 [64, 64], replicated
- w_k: bfloat16 [64, 64], replicated
- w_v: bfloat16 [64, 64], replicated
- w_b: bfloat16 [64, 4], replicated
- w_g: bfloat16 [64, 64], replicated
- w_o: bfloat16 [64, 64], replicated
Outputs:
- output: bfloat16 [1024, 1024, 64], P(('data', 'row'), 'col')
All inputs are finite; a program needn't handle non-finite values.
Results may differ from the reference program's by a relative error of at most 0.00643641.
Values are sent between devices in bfloat16 or wider.
A program may use at most 1 GiB of HBM per device.

```python
import math
import jax
import jax.numpy as jnp
from jax import lax

N = 1024
C_Z = 64
HEADS = 4
HEAD = 16

PROJ = HEADS * HEAD
Q_SCALE = 1.0 / math.sqrt(HEAD)
LN_EPS = 1e-5
MASK_FILL = -1e9
OUT_GAIN = 0.35 * math.sqrt(N / PROJ)


def setup_inputs(seed: int = 0, part: int = 0) -> dict:
    base_key = jax.random.key(seed)
    part_key = jax.random.fold_in(base_key, part)
    key_pair, key_len = jax.random.split(part_key, 2)
    pair_rep = jax.random.normal(key_pair, (N, N, C_Z), jnp.float32).astype(jnp.bfloat16)
    pad_len = jax.random.randint(key_len, (), N // 16, N // 4 + 1)
    res_mask = (jnp.arange(N) < N - pad_len).astype(jnp.int32)
    weight_keys = jax.random.split(base_key, 8)
    in_scale = 1.0 / math.sqrt(C_Z)
    ln_gamma = jax.random.uniform(weight_keys[0], (C_Z,), jnp.float32, 0.5, 1.5)
    ln_beta = 0.1 * jax.random.normal(weight_keys[1], (C_Z,), jnp.float32)
    w_q = (in_scale * jax.random.normal(weight_keys[2], (C_Z, PROJ), jnp.float32)).astype(jnp.bfloat16)
    w_k = (in_scale * jax.random.normal(weight_keys[3], (C_Z, PROJ), jnp.float32)).astype(jnp.bfloat16)
    w_v = (in_scale * jax.random.normal(weight_keys[4], (C_Z, PROJ), jnp.float32)).astype(jnp.bfloat16)
    w_b = (in_scale * jax.random.normal(weight_keys[5], (C_Z, HEADS), jnp.float32)).astype(jnp.bfloat16)
    w_g = (in_scale * jax.random.normal(weight_keys[6], (C_Z, PROJ), jnp.float32)).astype(jnp.bfloat16)
    w_o = (OUT_GAIN * jax.random.normal(weight_keys[7], (PROJ, C_Z), jnp.float32)).astype(jnp.bfloat16)
    return {'pair_rep': pair_rep, 'res_mask': res_mask, 'ln_gamma': ln_gamma, 'ln_beta': ln_beta, 'w_q': w_q, 'w_k': w_k, 'w_v': w_v, 'w_b': w_b, 'w_g': w_g, 'w_o': w_o}


def reference(pair_rep, res_mask, ln_gamma, ln_beta, w_q, w_k, w_v, w_b, w_g, w_o):
    pair_f32 = pair_rep.astype(jnp.float32)
    mean = jnp.mean(pair_f32, axis=-1, keepdims=True)
    centred = pair_f32 - mean
    variance = jnp.mean(centred * centred, axis=-1, keepdims=True)
    normed = (centred * lax.rsqrt(variance + LN_EPS) * ln_gamma + ln_beta).astype(jnp.bfloat16)
    bias = jnp.dot(normed.reshape(N * N, C_Z), w_b, preferred_element_type=jnp.float32).astype(jnp.bfloat16).reshape(N, N, HEADS)
    key_fill = jnp.where(res_mask > 0, 0.0, MASK_FILL).astype(jnp.float32)
    bias_ik = jnp.transpose(bias, (1, 0, 2)).astype(jnp.float32) + key_fill[None, :, None]

    def one_column(col_args):
        a_col, z_col = col_args
        query = (jnp.dot(a_col, w_q, preferred_element_type=jnp.float32) * Q_SCALE).astype(jnp.bfloat16).reshape(N, HEADS, HEAD)
        keys = jnp.dot(a_col, w_k, preferred_element_type=jnp.float32).astype(jnp.bfloat16).reshape(N, HEADS, HEAD)
        values = jnp.dot(a_col, w_v, preferred_element_type=jnp.float32).astype(jnp.bfloat16).reshape(N, HEADS, HEAD)
        gate = jax.nn.sigmoid(jnp.dot(a_col, w_g, preferred_element_type=jnp.float32))
        logits = jnp.einsum('ihd,khd->ikh', query.astype(jnp.float32), keys.astype(jnp.float32)) + bias_ik
        attn_prob = jax.nn.softmax(logits, axis=1)
        attended = jnp.einsum('ikh,khd->ihd', attn_prob, values.astype(jnp.float32)).reshape(N, PROJ)
        gated = (gate * attended).astype(jnp.bfloat16)
        return (z_col.astype(jnp.float32) + jnp.dot(gated, w_o, preferred_element_type=jnp.float32)).astype(jnp.bfloat16)

    out_cols = lax.map(one_column, (jnp.transpose(normed, (1, 0, 2)), jnp.transpose(pair_rep, (1, 0, 2))))
    return jnp.transpose(out_cols, (1, 0, 2))
```

```python
import functools
import math
import jax
import jax.numpy as jnp
from jax import lax
from jax.experimental import pallas as pl
from jax.experimental.pallas import tpu as pltpu
from jax.sharding import PartitionSpec as P

LN_EPS = 1e-5
LOG2E = math.log2(math.e)
FILL_PARTS = (-998244352.0, -1753088.0, -2560.0)
J, C, R, H, D = 16, 64, 512, 4, 16
NIB = 4
MESH = pl.DeviceIdType.MESH
BF, F32 = jnp.bfloat16, jnp.float32
PARTS = ((0, 3), (3, 3), (6, 2))
ORDERS = (("x", "y", "z"), ("y", "z", "x"), ("z", "x", "y"))
GROUPS = 2


class Gather:
    def __init__(self, bias_all, send_sem, recv_sem):
        self.buf, self.send_sem, self.recv_sem = bias_all, send_sem, recv_sem
        self.col, self.row = lax.axis_index("col"), lax.axis_index("row")
        self.z, self.y, self.x = self.col // 16, (self.col // 4) % 4, self.col % 4
        self.turn = (self.z - 2 * self.row + 4) % 4
        self.source = self.turn < 2

    def neighbour(self, dim, step):
        z, y, x = self.z, self.y, self.x
        if dim == "z":
            z = (z + step + 4) % 4
        elif dim == "y":
            y = (y + step + 4) % 4
        else:
            x = (x + step + 4) % 4
        return {"col": (z * 4 + y) * 4 + x, "row": self.row}

    def view(self, group, part, phase, value, head):
        order = ORDERS[part]
        pos = {}
        for n, dim in enumerate(order):
            if n < phase:
                pos[dim] = slice(None)
            elif n == phase:
                pos[dim] = value
            else:
                pos[dim] = {"z": self.z % 2, "y": self.y, "x": self.x}[dim]
        lo, size = PARTS[part]
        first = group * 2 if head is None else group * 2 + head
        return self.buf.at[pl.ds(first, 2 if head is None else 1), pl.ds(lo, size), pos["z"], pos["y"], pos["x"]]

    def copy(self, group, part, phase, slot, value, head, step):
        dim = ORDERS[part][phase]
        sem = ((group * 3 + part) * 3 + phase) * 4 + slot
        ref = self.view(group, part, phase, value, head)
        return pltpu.make_async_remote_copy(src_ref=ref, dst_ref=ref, send_sem=self.send_sem.at[sem], recv_sem=self.recv_sem.at[sem], device_id=self.neighbour(dim, step), device_id_type=MESH)

    def here(self, dim):
        return {"z": self.z % 2, "y": self.y, "x": self.x}[dim]

    def first(self, group, part, phase, act):
        order = ORDERS[part]
        dim = order[phase]

        def go():
            for slot, step in ((0, 1), (1, -1)):
                getattr(self.copy(group, part, phase, slot, self.here(dim), None, step), act)()

        if "z" in order[phase:]:
            pl.when(self.source)(go)
        else:
            go()

    def relay(self, group, part, phase, act):
        order = ORDERS[part]
        dim = order[phase]
        if dim == "z":
            cases = ((0, 1, 1, 0, -1, 3), (1, 0, 0, 0, 1, 2), (2, 0, 1, 1, 1, 2), (3, 1, 0, 1, -1, 3))
            for turn, slot, value, head, step, out in cases:

                @pl.when(self.turn == turn)
                def _():
                    if act == "start":
                        self.copy(group, part, phase, slot, value, None, 1).wait_recv()
                    getattr(self.copy(group, part, phase, out, value, head, step), act)()

            return

        def go():
            here = self.here(dim)
            behind, ahead = (here + 3) % 4, (here + 1) % 4
            if act == "start":
                self.copy(group, part, phase, 0, behind, None, 1).wait_recv()
            getattr(self.copy(group, part, phase, 2, behind, 0, 1), act)()
            if act == "start":
                self.copy(group, part, phase, 1, ahead, None, -1).wait_recv()
            getattr(self.copy(group, part, phase, 3, ahead, 1, -1), act)()

        if "z" in order[phase:]:
            pl.when(self.source)(go)
        else:
            go()

    def finish(self, group, part, phase):
        order = ORDERS[part]
        dim = order[phase]
        if dim == "z":
            for turn, value, slots in ((2, 0, ((2, 0), (3, 1))), (3, 1, ((3, 0), (2, 1)))):

                @pl.when(self.turn == turn)
                def _():
                    for slot, head in slots:
                        self.copy(group, part, phase, slot, value, head, 1).wait_recv()

            return

        def go():
            far = (self.here(dim) + 2) % 4
            self.copy(group, part, phase, 2, far, 0, 1).wait_recv()
            self.copy(group, part, phase, 3, far, 1, -1).wait_recv()

        if "z" in order[phase:]:
            pl.when(self.source)(go)
        else:
            go()

    def everywhere(self, method, phase, *extra, groups=range(GROUPS)):
        for group in groups:
            for part in range(3):
                method(group, part, phase, *extra)


def kernel(pair_ref, mask_ref, gamma_ref, beta_ref, wt_ref, wbt_ref, wot_ref, out_ref,
           normed, bias_f32, bias_own, bias_all, query, keys_t, keys, values, gate, gated, const, fill_rows, bias_kt, logits,
           send_sem, recv_sem, own_send, own_recv, kv_send, kv_recv):
    row = lax.axis_index("row")
    gather = Gather(bias_all, send_sem, recv_sem)
    owner = gather.z // 2
    partner = {"row": 1 - row}

    barrier = pltpu.get_barrier_semaphore()
    peers = [partner] + [gather.neighbour(dim, step) for dim in "xyz" for step in (1, -1)]
    for peer in peers:
        pl.semaphore_signal(barrier, inc=1, device_id=peer, device_id_type=MESH)

    gamma, beta = gamma_ref[...], beta_ref[...]
    wbt = wbt_ref[...]
    for j in range(J):
        pair = pair_ref[j].astype(F32)
        mean = jnp.mean(pair, axis=0, keepdims=True)
        centred = pair - mean
        variance = jnp.mean(centred * centred, axis=0, keepdims=True)
        a = (centred * lax.rsqrt(variance + LN_EPS) * gamma + beta).astype(BF)
        normed[j] = a
        b = jnp.dot(wbt, a, preferred_element_type=F32)
        for h in range(H):
            bias_f32[h, j:j + 1, :] = b[h:h + 1, :]
    for h in range(H):
        for t in range(4):
            bias_own[h, t] = bias_f32[h, :, t * 128:(t + 1) * 128].astype(BF)

    pl.semaphore_wait(barrier, len(peers))

    def own_place(r):
        return bias_all.at[:, pl.ds(r * 4, 4), gather.z % 2, gather.y, gather.x]

    def own_away():
        return pltpu.make_async_remote_copy(src_ref=bias_own, dst_ref=own_place(row), send_sem=own_send.at[0], recv_sem=own_recv.at[0], device_id=partner, device_id_type=MESH)

    def own_stay():
        return pltpu.make_async_copy(bias_own, own_place(row), own_send.at[1])

    @pl.when(row != owner)
    def _():
        own_away().start()

    @pl.when(row == owner)
    def _():
        own_stay().start()
        own_stay().wait()
        pltpu.make_async_remote_copy(src_ref=bias_own, dst_ref=own_place(1 - row), send_sem=own_send.at[0], recv_sem=own_recv.at[0], device_id=partner, device_id_type=MESH).wait_recv()

    gather.everywhere(gather.first, 0, "start")

    rows_i = lax.broadcasted_iota(jnp.int32, (64, 256), 0)
    const[0:64, :] = jnp.where(rows_i < 3, 1.0, 0.0).astype(BF)
    eye_r = lax.broadcasted_iota(jnp.int32, (128, 256), 0)
    eye_c = lax.broadcasted_iota(jnp.int32, (128, 256), 1)
    const[64:192, :] = jnp.where((eye_c == eye_r) | (eye_c == eye_r + 128), 1.0, 0.0).astype(BF)
    shut = jnp.where(mask_ref[pl.ds(row, 1), :] > 0, 0.0, 1.0)
    piece = lax.broadcasted_iota(jnp.int32, (64, R), 0)
    fill = jnp.where(piece == 0, FILL_PARTS[0], jnp.where(piece == 1, FILL_PARTS[1], jnp.where(piece == 2, FILL_PARTS[2], 0.0)))
    fill_rows[...] = (fill * shut).astype(BF)

    wt = wt_ref[...]

    def project(j, carry):
        r = jnp.dot(wt, normed[j], preferred_element_type=F32)
        q = (r[0:64] * (1.0 / math.sqrt(D))).astype(BF)
        k = r[64:128].astype(BF)
        v = r[128:192].astype(BF)
        g = jax.nn.sigmoid(r[192:256])
        for h in range(H):
            sl = slice(h * D, (h + 1) * D)
            keys_t[h, j] = k[sl]
            values[row, h, j] = v[sl]
            for ib in range(NIB):
                query[h, ib, j] = q[sl, ib * 128:(ib + 1) * 128]
                gate[h, ib, j] = g[sl, ib * 128:(ib + 1) * 128]
        return carry

    lax.fori_loop(0, 8, project, 0)
    gather.everywhere(gather.relay, 0, "start")
    lax.fori_loop(8, 16, project, 0)
    gather.everywhere(gather.finish, 0)
    gather.everywhere(gather.first, 1, "start")

    def turn_keys(n, carry):
        kt = keys_t[n // 4, pl.ds((n % 4) * 4, 4)].reshape(64, R)
        full = jnp.concatenate([kt, fill_rows[...]], axis=0)
        keys[row, n] = full.T
        return carry

    lax.fori_loop(0, 16, turn_keys, 0)

    def kv_copy(which):
        ref = (keys if which == 0 else values).at[row]
        return pltpu.make_async_remote_copy(src_ref=ref, dst_ref=ref, send_sem=kv_send.at[which], recv_sem=kv_recv.at[which], device_id=partner, device_id_type=MESH)

    kv_copy(1).start()
    gather.everywhere(gather.relay, 1, "start")
    kv_copy(0).start()
    gather.everywhere(gather.finish, 1)
    gather.everywhere(gather.first, 2, "start")
    for which in (0, 1):
        ref = (keys if which == 0 else values).at[1 - row]
        pltpu.make_async_remote_copy(src_ref=ref, dst_ref=ref, send_sem=kv_send.at[which], recv_sem=kv_recv.at[which], device_id=partner, device_id_type=MESH).wait_recv()
    gather.everywhere(gather.relay, 2, "start", groups=(0,))
    gather.everywhere(gather.finish, 2, groups=(0,))

    attend_heads(0, bias_all, query, keys, values, gate, gated, const, bias_kt, logits,
                 after_first=lambda: gather.everywhere(gather.relay, 2, "start", groups=(1,)))
    gather.everywhere(gather.finish, 2, groups=(1,))
    attend_heads(2, bias_all, query, keys, values, gate, gated, const, bias_kt, logits)
    project_out(pair_ref, wot_ref, gated, out_ref)

    for phase in range(3):
        gather.everywhere(gather.first, phase, "wait_send")
        gather.everywhere(gather.relay, phase, "wait_send")
    kv_copy(0).wait_send()
    kv_copy(1).wait_send()

    @pl.when(row != owner)
    def _():
        own_away().wait_send()


def attend_heads(head_lo, bias_all, query, keys, values, gate, gated, const, bias_kt, logits, after_first=None):
    def unit(n):
        h, ib = head_lo + n // NIB, n % NIB
        for t in range(8):
            block = bias_all[h, t, ib // 2, pl.ds((ib % 2) * 2, 2)].reshape(128, 128)
            bias_kt[t * 128:(t + 1) * 128, :] = block.T

        def score(p):
            group, odd = p // 2, p % 2
            zero = jnp.zeros((16, 128), BF)
            gap = jnp.zeros((16, 256), BF)
            left = jnp.concatenate([query[h, ib, 2 * p], zero], axis=1)
            right = jnp.concatenate([zero, query[h, ib, 2 * p + 1]], axis=1)
            top = [gap, gap, left, right] if odd else [left, right, gap, gap]
            rhs = jnp.concatenate(top + [const[...]], axis=0)
            best = None
            for kh in range(2):
                lhs = jnp.concatenate([keys[kh, h * 4 + group], bias_kt[kh * R:(kh + 1) * R, :]], axis=1)
                s = jnp.dot(lhs, rhs, preferred_element_type=F32)
                logits[p % 2, kh * R:(kh + 1) * R, :] = s
                m = jnp.max(s, axis=0, keepdims=True)
                best = m if best is None else jnp.maximum(best, m)
            return best

        def mix(p, best):
            total = jnp.zeros((1, 256), F32)
            acc = None
            for kh in range(2):
                e = jnp.exp2((logits[p % 2, kh * R:(kh + 1) * R, :] - best) * LOG2E)
                total = total + jnp.sum(e, axis=0, keepdims=True)
                v = jnp.concatenate([values[kh, h, 2 * p], values[kh, h, 2 * p + 1]], axis=0)
                o = jnp.dot(v, e.astype(BF), preferred_element_type=F32)
                acc = o if acc is None else acc + o
            scale = 1.0 / total
            gated[ib, 2 * p, h] = (gate[h, ib, 2 * p] * (acc[0:16, 0:128] * scale[:, 0:128])).astype(BF)
            gated[ib, 2 * p + 1, h] = (gate[h, ib, 2 * p + 1] * (acc[16:32, 128:256] * scale[:, 128:256])).astype(BF)

        best = score(0)
        for p in range(8):
            later = score(p + 1) if p < 7 else None
            mix(p, best)
            best = later

    if after_first is None:
        pl.loop(0, 2 * NIB)(unit)
    else:
        pl.loop(0, 1)(unit)
        after_first()
        pl.loop(1, 2 * NIB)(unit)


def project_out(pair_ref, wot_ref, gated, out_ref):
    wot = wot_ref[...]

    def one(j, carry):
        g = jnp.concatenate([gated[ib, j].reshape(64, 128) for ib in range(NIB)], axis=1)
        update = jnp.dot(wot, g, preferred_element_type=F32)
        out_ref[j] = (pair_ref[j].astype(F32) + update).astype(BF)
        return carry

    lax.fori_loop(0, J, one, 0)


SCRATCH = dict(
    normed=((J, C, R), BF), bias_f32=((H, J, R), F32), bias_own=((H, 4, J, 128), BF), bias_all=((H, 8, 2, 4, 4, J, 128), BF),
    query=((H, NIB, J, D, 128), BF), keys_t=((H, J, D, R), BF), keys=((2, 16, R, 128), BF), values=((2, H, J, D, R), BF),
    gate=((H, NIB, J, D, 128), F32), gated=((NIB, J, H, D, 128), BF), const=((192, 256), BF), fill_rows=((64, R), BF),
    bias_kt=((2 * R, 128), BF), logits=((2, 2 * R, 256), F32))


def solution(mesh):
    def body(pair_tile, res_mask, ln_gamma, ln_beta, w_q, w_k, w_v, w_b, w_g, w_o):
        pair_t = jnp.transpose(pair_tile, (1, 2, 0))
        wt = jnp.concatenate([w_q, w_k, w_v, w_g], axis=1).T
        wbt = jnp.pad(w_b.T, ((0, 4), (0, 0)))
        scratch = [pltpu.VMEM(shape, dtype) for shape, dtype in SCRATCH.values()]
        sems = [pltpu.SemaphoreType.DMA((GROUPS * 36,)), pltpu.SemaphoreType.DMA((GROUPS * 36,)), pltpu.SemaphoreType.DMA((2,)), pltpu.SemaphoreType.DMA((2,)), pltpu.SemaphoreType.DMA((2,)), pltpu.SemaphoreType.DMA((2,))]
        out_t = pl.pallas_call(
            kernel,
            out_shape=jax.ShapeDtypeStruct((J, C, R), BF),
            in_specs=[pl.BlockSpec(memory_space=pltpu.VMEM)] * 7,
            out_specs=pl.BlockSpec(memory_space=pltpu.VMEM),
            scratch_shapes=scratch + sems,
            compiler_params=pltpu.CompilerParams(collective_id=0, has_side_effects=True, vmem_limit_bytes=60 * 1024 * 1024),
        )(pair_t, res_mask.reshape(2, R), ln_gamma.reshape(C, 1), ln_beta.reshape(C, 1), wt, wbt, w_o.T)
        return jnp.transpose(out_t, (2, 0, 1))

    tile_spec = P(("data", "row"), "col", None)
    return jax.shard_map(body, mesh=mesh, in_specs=(tile_spec, P("data"), P(), P(), P(), P(), P(), P(), P(), P()), out_specs=tile_spec, check_vma=False)
```

```python
import functools
import math
import jax
import jax.numpy as jnp
from jax import lax
from jax.experimental import pallas as pl
from jax.experimental.pallas import tpu as pltpu
from jax.sharding import PartitionSpec as P

LN_EPS = 1e-5
LOG2E = math.log2(math.e)
FILL_PARTS = (-998244352.0, -1753088.0, -2560.0)
J, C, R, H, D = 16, 64, 512, 4, 16
NIB = 4
MESH = pl.DeviceIdType.MESH
BF, F32 = jnp.bfloat16, jnp.float32
PARTS = ((0, 3), (3, 3), (6, 2))
ORDERS = (("x", "y", "z"), ("y", "z", "x"), ("z", "x", "y"))


class Gather:
    def __init__(self, bias_all, send_sem, recv_sem):
        self.buf, self.send_sem, self.recv_sem = bias_all, send_sem, recv_sem
        self.col, self.row = lax.axis_index("col"), lax.axis_index("row")
        self.z, self.y, self.x = self.col // 16, (self.col // 4) % 4, self.col % 4
        self.turn = (self.z - 2 * self.row + 4) % 4
        self.source = self.turn < 2

    def neighbour(self, dim, step):
        z, y, x = self.z, self.y, self.x
        if dim == "z":
            z = (z + step + 4) % 4
        elif dim == "y":
            y = (y + step + 4) % 4
        else:
            x = (x + step + 4) % 4
        return {"col": (z * 4 + y) * 4 + x, "row": self.row}

    def here(self, dim):
        return {"z": self.z % 2, "y": self.y, "x": self.x}[dim]

    def copy(self, head, part, phase, slot, value, half, step):
        order = ORDERS[part]
        pos = {}
        for n, dim in enumerate(order):
            pos[dim] = slice(None) if n < phase else value if n == phase else self.here(dim)
        if half is not None:
            dim, size = ("y", 2) if part == 0 else ("z", 1)
            pos[dim] = pl.ds(half * size, size)
        lo, size = PARTS[part]
        ref = self.buf.at[head, pl.ds(lo, size), pos["z"], pos["y"], pos["x"]]
        sem = ((head * 3 + part) * 3 + phase) * 4 + slot
        return pltpu.make_async_remote_copy(src_ref=ref, dst_ref=ref, send_sem=self.send_sem.at[sem], recv_sem=self.recv_sem.at[sem], device_id=self.neighbour(order[phase], step), device_id_type=MESH)

    def among(self, part, phase, go):
        pl.when(self.source)(go) if "z" in ORDERS[part][phase:] else go()

    def first(self, head, phase, act="start"):
        for part in range(3):

            def go():
                for slot, step in ((0, 1), (1, -1), (2, 2))[: 2 if phase == 2 else 3]:
                    getattr(self.copy(head, part, phase, slot, self.here(ORDERS[part][phase]), None, step), act)()

            self.among(part, phase, go)

    def arrived(self, head, phase):
        for part in range(3):
            dim = ORDERS[part][phase]
            if dim == "z":
                for turn, waits in enumerate((((1, 1),), ((0, 0),), ((0, 1), (2, 0)), ((1, 0), (2, 1)))):

                    @pl.when(self.turn == turn)
                    def _():
                        for slot, value in waits:
                            self.copy(head, part, phase, slot, value, None, 1).wait_recv()

                continue

            def go():
                for slot, back in ((0, 3), (1, 1), (2, 2)):
                    self.copy(head, part, phase, slot, (self.here(dim) + back) % 4, None, 1).wait_recv()

            self.among(part, phase, go)

    def relay(self, head, act="start"):
        for part in range(3):
            dim = ORDERS[part][2]
            if dim == "z":
                cases = ((0, 1, 1, 0, -1, 3), (1, 0, 0, 0, 1, 2), (2, 0, 1, 1, 1, 2), (3, 1, 0, 1, -1, 3))
                for turn, slot, value, half, step, out in cases:

                    @pl.when(self.turn == turn)
                    def _():
                        if act == "start":
                            self.copy(head, part, 2, slot, value, None, 1).wait_recv()
                        getattr(self.copy(head, part, 2, out, value, half, step), act)()

                continue
            for slot, back, half, step in ((0, 3, 0, 1), (1, 1, 1, -1)):
                value = (self.here(dim) + back) % 4
                if act == "start":
                    self.copy(head, part, 2, slot, value, None, 1).wait_recv()
                getattr(self.copy(head, part, 2, slot + 2, value, half, step), act)()

    def finish(self, head):
        for part in range(3):
            dim = ORDERS[part][2]
            if dim == "z":
                for turn, value, slots in ((2, 0, ((2, 0), (3, 1))), (3, 1, ((3, 0), (2, 1)))):

                    @pl.when(self.turn == turn)
                    def _():
                        for slot, half in slots:
                            self.copy(head, part, 2, slot, value, half, 1).wait_recv()

                continue
            for slot, half in ((2, 0), (3, 1)):
                self.copy(head, part, 2, slot, (self.here(dim) + 2) % 4, half, 1).wait_recv()

    def step1(self, head):
        self.arrived(head, 0)
        self.first(head, 1)

    def step2(self, head):
        self.arrived(head, 1)
        self.first(head, 2)


def kernel(pair_ref, mask_ref, gamma_ref, beta_ref, wq_ref, wk_ref, wv_ref, wg_ref, wbt_ref, wo_ref, out_ref,
           normed, bias_f32, bias_own, bias_all, query, keys_t, keys, values, gate, gated, const, fill_rows, weights, bias_kt, logits,
           send_sem, recv_sem, own_send, own_recv, kv_send, kv_recv):
    row = lax.axis_index("row")
    gather = Gather(bias_all, send_sem, recv_sem)
    owner = gather.z // 2
    partner = {"row": 1 - row}

    barrier = pltpu.get_barrier_semaphore()
    peers = [partner] + [gather.neighbour(dim, step) for dim in "xyz" for step in (1, -1, 2)]
    for peer in peers:
        pl.semaphore_signal(barrier, inc=1, device_id=peer, device_id_type=MESH)

    diag = lax.broadcasted_iota(jnp.int32, (C, C), 0) == lax.broadcasted_iota(jnp.int32, (C, C), 1)
    gamma = jnp.sum(jnp.where(diag, gamma_ref[...], 0.0), axis=1, keepdims=True)
    beta = jnp.sum(jnp.where(diag, beta_ref[...], 0.0), axis=1, keepdims=True)
    wbt = wbt_ref[...]
    for j in range(J):
        pair = pair_ref[j].astype(F32)
        mean = jnp.mean(pair, axis=0, keepdims=True)
        centred = pair - mean
        variance = jnp.mean(centred * centred, axis=0, keepdims=True)
        a = (centred * lax.rsqrt(variance + LN_EPS) * gamma + beta).astype(BF)
        normed[j] = a
        b = jnp.dot(wbt, a, preferred_element_type=F32)
        for h in range(H):
            bias_f32[h, j:j + 1, :] = b[h:h + 1, :]
    for h in range(H):
        for t in range(4):
            bias_own[h, t] = bias_f32[h, :, t * 128:(t + 1) * 128].astype(BF)

    pl.semaphore_wait(barrier, len(peers))

    def own_place(r):
        return bias_all.at[:, pl.ds(r * 4, 4), gather.z % 2, gather.y, gather.x]

    def own_away():
        return pltpu.make_async_remote_copy(src_ref=bias_own, dst_ref=own_place(row), send_sem=own_send.at[0], recv_sem=own_recv.at[0], device_id=partner, device_id_type=MESH)

    def own_stay():
        return pltpu.make_async_copy(bias_own, own_place(row), own_send.at[1])

    @pl.when(row != owner)
    def _():
        own_away().start()

    @pl.when(row == owner)
    def _():
        own_stay().start()
        own_stay().wait()
        pltpu.make_async_remote_copy(src_ref=bias_own, dst_ref=own_place(1 - row), send_sem=own_send.at[0], recv_sem=own_recv.at[0], device_id=partner, device_id_type=MESH).wait_recv()

    for h in range(H):
        gather.first(h, 0)

    rows_i = lax.broadcasted_iota(jnp.int32, (64, 256), 0)
    const[0:64, :] = jnp.where(rows_i < 3, 1.0, 0.0).astype(BF)
    eye_r = lax.broadcasted_iota(jnp.int32, (128, 256), 0)
    eye_c = lax.broadcasted_iota(jnp.int32, (128, 256), 1)
    const[64:192, :] = jnp.where((eye_c == eye_r) | (eye_c == eye_r + 128), 1.0, 0.0).astype(BF)
    piece = lax.broadcasted_iota(jnp.int32, (64, 128), 0)
    fill = jnp.where(piece == 0, FILL_PARTS[0], jnp.where(piece == 1, FILL_PARTS[1], jnp.where(piece == 2, FILL_PARTS[2], 0.0)))
    for t in range(4):
        shut = jnp.where(mask_ref[pl.ds(row * 4 + t, 1), :] > 0, 0.0, 1.0)
        fill_rows[:, t * 128:(t + 1) * 128] = (fill * shut).astype(BF)
    for n, w_ref in enumerate((wq_ref, wk_ref, wv_ref, wg_ref, wo_ref)):
        weights[n * C:(n + 1) * C, :] = w_ref[...].T
    wt = weights[0:4 * C, :]

    def project(j, carry):
        r = jnp.dot(wt, normed[j], preferred_element_type=F32)
        q = (r[0:64] * (1.0 / math.sqrt(D))).astype(BF)
        k = r[64:128].astype(BF)
        v = r[128:192].astype(BF)
        g = jax.nn.sigmoid(r[192:256])
        for h in range(H):
            sl = slice(h * D, (h + 1) * D)
            keys_t[h, j] = k[sl]
            values[row, h, j] = v[sl]
            for ib in range(NIB):
                query[h, ib, j] = q[sl, ib * 128:(ib + 1) * 128]
                gate[h, ib, j] = g[sl, ib * 128:(ib + 1) * 128]
        return carry

    def turn_keys(n, carry):
        kt = keys_t[n // 4, pl.ds((n % 4) * 4, 4)].reshape(64, R)
        full = jnp.concatenate([kt, fill_rows[...]], axis=0)
        keys[row, n] = full.T
        return carry

    def kv_copies(h, r):
        for n, ref in enumerate((keys.at[r, pl.ds(h * 4, 4)], values.at[r, h])):
            yield pltpu.make_async_remote_copy(src_ref=ref, dst_ref=ref, send_sem=kv_send.at[h * 2 + n], recv_sem=kv_recv.at[h * 2 + n], device_id=partner, device_id_type=MESH)

    lax.fori_loop(0, 8, project, 0)
    gather.step1(0)
    lax.fori_loop(8, 16, project, 0)
    gather.step2(0)
    gather.step1(1)
    lax.fori_loop(0, 16, turn_keys, 0)
    for h in range(H):
        for copy in kv_copies(h, row):
            copy.start()
    gather.relay(0)
    gather.step2(1)

    @pl.loop(0, H * NIB)
    def _(n):
        h, ib = n // NIB, n % NIB

        @pl.when(ib == 0)
        def _():
            for copy in kv_copies(h, 1 - row):
                copy.wait_recv()
            gather.finish(h)

        @pl.when((ib == 0) & (h < H - 2))
        def _():
            gather.step1(h + 2)

        @pl.when((ib == 1) & (h < H - 1))
        def _():
            gather.relay(h + 1)

        @pl.when((ib == 2) & (h < H - 2))
        def _():
            gather.step2(h + 2)

        attend(h, ib, bias_all, query, keys, values, gate, gated, const, bias_kt, logits)

    project_out(pair_ref, weights, gated, out_ref)

    @pl.loop(0, H)
    def _(h):
        for phase in range(3):
            gather.first(h, phase, "wait_send")
        gather.relay(h, "wait_send")
        for copy in kv_copies(h, row):
            copy.wait_send()

    @pl.when(row != owner)
    def _():
        own_away().wait_send()


def attend(h, ib, bias_all, query, keys, values, gate, gated, const, bias_kt, logits):
    for t in range(8):
        block = bias_all[h, t, ib // 2, pl.ds((ib % 2) * 2, 2)].reshape(128, 128)
        bias_kt[t * 128:(t + 1) * 128, :] = block.T

    def score(p):
        group, odd = p // 2, p % 2
        zero = jnp.zeros((16, 128), BF)
        gap = jnp.zeros((16, 256), BF)
        left = jnp.concatenate([query[h, ib, 2 * p], zero], axis=1)
        right = jnp.concatenate([zero, query[h, ib, 2 * p + 1]], axis=1)
        top = [gap, gap, left, right] if odd else [left, right, gap, gap]
        rhs = jnp.concatenate(top + [const[...]], axis=0)
        best = None
        for kh in range(2):
            lhs = jnp.concatenate([keys[kh, h * 4 + group], bias_kt[kh * R:(kh + 1) * R, :]], axis=1)
            s = jnp.dot(lhs, rhs, preferred_element_type=F32)
            logits[p % 2, kh * R:(kh + 1) * R, :] = s
            m = jnp.max(s, axis=0, keepdims=True)
            best = m if best is None else jnp.maximum(best, m)
        return best

    def mix(p, best):
        total = jnp.zeros((1, 256), F32)
        acc = None
        for kh in range(2):
            e = jnp.exp2((logits[p % 2, kh * R:(kh + 1) * R, :] - best) * LOG2E)
            total = total + jnp.sum(e, axis=0, keepdims=True)
            v = jnp.concatenate([values[kh, h, 2 * p], values[kh, h, 2 * p + 1]], axis=0)
            o = jnp.dot(v, e.astype(BF), preferred_element_type=F32)
            acc = o if acc is None else acc + o
        scale = 1.0 / total
        gated[ib, 2 * p, h] = (gate[h, ib, 2 * p] * (acc[0:16, 0:128] * scale[:, 0:128])).astype(BF)
        gated[ib, 2 * p + 1, h] = (gate[h, ib, 2 * p + 1] * (acc[16:32, 128:256] * scale[:, 128:256])).astype(BF)

    best = score(0)
    for p in range(8):
        later = score(p + 1) if p < 7 else None
        mix(p, best)
        best = later


def project_out(pair_ref, weights, gated, out_ref):
    wot = weights[4 * C:5 * C, :]

    def one(j, carry):
        g = jnp.concatenate([gated[ib, j].reshape(64, 128) for ib in range(NIB)], axis=1)
        update = jnp.dot(wot, g, preferred_element_type=F32)
        out_ref[j] = (pair_ref[j].astype(F32) + update).astype(BF)
        return carry

    lax.fori_loop(0, J, one, 0)


SCRATCH = dict(
    normed=((J, C, R), BF), bias_f32=((H, J, R), F32), bias_own=((H, 4, J, 128), BF), bias_all=((H, 8, 2, 4, 4, J, 128), BF),
    query=((H, NIB, J, D, 128), BF), keys_t=((H, J, D, R), BF), keys=((2, 16, R, 128), BF), values=((2, H, J, D, R), BF),
    gate=((H, NIB, J, D, 128), F32), gated=((NIB, J, H, D, 128), BF), const=((192, 256), BF), fill_rows=((64, R), BF), weights=((5 * C, C), BF),
    bias_kt=((2 * R, 128), BF), logits=((2, 2 * R, 256), F32))


def solution(mesh):
    def body(pair_tile, res_mask, ln_gamma, ln_beta, w_q, w_k, w_v, w_b, w_g, w_o):
        pair_t = jnp.transpose(pair_tile, (1, 2, 0))
        scratch = [pltpu.VMEM(shape, dtype) for shape, dtype in SCRATCH.values()]
        sems = [pltpu.SemaphoreType.DMA((n,)) for n in (H * 36, H * 36, 2, 1, 2 * H, 2 * H)]
        out_t = pl.pallas_call(
            kernel,
            out_shape=jax.ShapeDtypeStruct((J, C, R), BF),
            in_specs=[pl.BlockSpec(memory_space=pltpu.VMEM)] * 10,
            out_specs=pl.BlockSpec(memory_space=pltpu.VMEM),
            scratch_shapes=scratch + sems,
            compiler_params=pltpu.CompilerParams(collective_id=0, has_side_effects=True, vmem_limit_bytes=60 * 1024 * 1024),
        )(pair_t, res_mask.reshape(8, 128), ln_gamma.reshape(1, C), ln_beta.reshape(1, C), w_q, w_k, w_v, w_g, w_b.T, w_o)
        return jnp.transpose(out_t, (2, 0, 1))

    tile_spec = P(("data", "row"), "col", None)
    return jax.shard_map(body, mesh=mesh, in_specs=(tile_spec, P("data"), P(), P(), P(), P(), P(), P(), P(), P()), out_specs=tile_spec, check_vma=False)
```

```python
import functools
import math
import jax
import jax.numpy as jnp
from jax import lax
from jax.experimental import pallas as pl
from jax.experimental.pallas import tpu as pltpu
from jax.sharding import PartitionSpec as P

LN_EPS = 1e-5
LOG2E = math.log2(math.e)
FILL_PARTS = (-998244352.0, -1753088.0, -2560.0)
J, C, R, H, D = 16, 64, 512, 4, 16
NIB = 4
MESH = pl.DeviceIdType.MESH
BF, F32 = jnp.bfloat16, jnp.float32
PARTS = ((0, 3), (3, 3), (6, 2))
ORDERS = (("x", "y", "z"), ("y", "z", "x"), ("z", "x", "y"))


class Gather:
    def __init__(self, bias_all, send_sem, recv_sem):
        self.bufs, self.send_sem, self.recv_sem = bias_all, send_sem, recv_sem
        self.col, self.row = lax.axis_index("col"), lax.axis_index("row")
        self.z, self.y, self.x = self.col // 16, (self.col // 4) % 4, self.col % 4
        self.turn = (self.z - 2 * self.row + 4) % 4
        self.source = self.turn < 2

    def neighbour(self, dim, step):
        z, y, x = self.z, self.y, self.x
        if dim == "z":
            z = (z + step + 4) % 4
        elif dim == "y":
            y = (y + step + 4) % 4
        else:
            x = (x + step + 4) % 4
        return {"col": (z * 4 + y) * 4 + x, "row": self.row}

    def here(self, dim):
        return {"z": self.z % 2, "y": self.y, "x": self.x}[dim]

    def copy(self, head, part, phase, slot, value, half, step):
        order = ORDERS[part]
        pos = {}
        for n, dim in enumerate(order):
            pos[dim] = slice(None) if n < phase else value if n == phase else self.here(dim)
        if half is not None:
            size = 1 if order[1] == "z" else 2
            pos[order[1]] = pl.ds(half * size, size)
        ref = self.bufs[part].at[(head, pos[order[2]], pos[order[1]], pos[order[0]])]
        sem = ((head * 3 + part) * 3 + phase) * 4 + slot
        return pltpu.make_async_remote_copy(src_ref=ref, dst_ref=ref, send_sem=self.send_sem.at[sem], recv_sem=self.recv_sem.at[sem], device_id=self.neighbour(order[phase], step), device_id_type=MESH)

    def among(self, part, phase, go):
        pl.when(self.source)(go) if "z" in ORDERS[part][phase:] else go()

    def first(self, head, phase, act="start"):
        for part in range(3):

            def go():
                for slot, step in ((0, 1), (1, -1), (2, 2))[: 2 if phase == 2 else 3]:
                    getattr(self.copy(head, part, phase, slot, self.here(ORDERS[part][phase]), None, step), act)()

            self.among(part, phase, go)

    def arrived(self, head, phase):
        for part in range(3):
            dim = ORDERS[part][phase]
            if dim == "z":
                for turn, waits in enumerate((((1, 1),), ((0, 0),), ((0, 1), (2, 0)), ((1, 0), (2, 1)))):

                    @pl.when(self.turn == turn)
                    def _():
                        for slot, value in waits:
                            self.copy(head, part, phase, slot, value, None, 1).wait_recv()

                continue

            def go():
                for slot, back in ((0, 3), (1, 1), (2, 2)):
                    self.copy(head, part, phase, slot, (self.here(dim) + back) % 4, None, 1).wait_recv()

            self.among(part, phase, go)

    def relay(self, head, act="start"):
        for part in range(3):
            dim = ORDERS[part][2]
            if dim == "z":
                cases = ((0, 1, 1, 0, -1, 3), (1, 0, 0, 0, 1, 2), (2, 0, 1, 1, 1, 2), (3, 1, 0, 1, -1, 3))
                for turn, slot, value, half, step, out in cases:

                    @pl.when(self.turn == turn)
                    def _():
                        if act == "start":
                            self.copy(head, part, 2, slot, value, None, 1).wait_recv()
                        getattr(self.copy(head, part, 2, out, value, half, step), act)()

                continue
            for slot, back, half, step in ((0, 3, 0, 1), (1, 1, 1, -1)):
                value = (self.here(dim) + back) % 4
                if act == "start":
                    self.copy(head, part, 2, slot, value, None, 1).wait_recv()
                getattr(self.copy(head, part, 2, slot + 2, value, half, step), act)()

    def finish(self, head):
        for part in range(3):
            dim = ORDERS[part][2]
            if dim == "z":
                for turn, value, slots in ((2, 0, ((2, 0), (3, 1))), (3, 1, ((3, 0), (2, 1)))):

                    @pl.when(self.turn == turn)
                    def _():
                        for slot, half in slots:
                            self.copy(head, part, 2, slot, value, half, 1).wait_recv()

                continue
            for slot, half in ((2, 0), (3, 1)):
                self.copy(head, part, 2, slot, (self.here(dim) + 2) % 4, half, 1).wait_recv()

    def step1(self, head):
        self.arrived(head, 0)
        self.first(head, 1)

    def step2(self, head):
        self.arrived(head, 1)
        self.first(head, 2)


def kernel(pair_ref, mask_ref, gamma_ref, beta_ref, wq_ref, wk_ref, wv_ref, wg_ref, wbt_ref, wo_ref, out_ref,
           normed, bias_f32, bias_own, bias_a, bias_b, bias_c, query, keys_t, keys, values, gate, gated, const, fill_rows, weights, bias_kt, logits, best,
           send_sem, recv_sem, own_send, own_recv, kv_send, kv_recv):
    row = lax.axis_index("row")
    bias_all = (bias_a, bias_b, bias_c)
    gather = Gather(bias_all, send_sem, recv_sem)
    owner = gather.z // 2
    partner = {"row": 1 - row}

    barrier = pltpu.get_barrier_semaphore()
    peers = [partner] + [gather.neighbour(dim, step) for dim in "xyz" for step in (1, -1, 2)]
    for peer in peers:
        pl.semaphore_signal(barrier, inc=1, device_id=peer, device_id_type=MESH)

    diag = lax.broadcasted_iota(jnp.int32, (C, C), 0) == lax.broadcasted_iota(jnp.int32, (C, C), 1)
    gamma = jnp.sum(jnp.where(diag, gamma_ref[...], 0.0), axis=1, keepdims=True)
    beta = jnp.sum(jnp.where(diag, beta_ref[...], 0.0), axis=1, keepdims=True)
    wbt = wbt_ref[...]
    for j in range(J):
        pair = pair_ref[j].astype(F32)
        mean = jnp.mean(pair, axis=0, keepdims=True)
        centred = pair - mean
        variance = jnp.mean(centred * centred, axis=0, keepdims=True)
        a = (centred * lax.rsqrt(variance + LN_EPS) * gamma + beta).astype(BF)
        normed[j] = a
        b = jnp.dot(wbt, a, preferred_element_type=F32)
        for h in range(H):
            bias_f32[h, j:j + 1, :] = b[h:h + 1, :]
    for h in range(H):
        for t in range(4):
            bias_own[h, t] = bias_f32[h, :, t * 128:(t + 1) * 128].astype(BF)

    pl.semaphore_wait(barrier, len(peers))

    def own_copies(r):
        for tiles, part, lo, size in (((0, 0, 0, 3), (3, 1, 0, 1)), ((0, 1, 1, 2), (2, 2, 0, 2)))[r]:
            place = tuple(gather.here(dim) for dim in reversed(ORDERS[part]))
            yield bias_own.at[:, pl.ds(tiles, size)], bias_all[part].at[(slice(None), *place, pl.ds(lo, size))]

    def own_away(r):
        for n, (src, dst) in enumerate(own_copies(r)):
            yield pltpu.make_async_remote_copy(src_ref=src, dst_ref=dst, send_sem=own_send.at[n], recv_sem=own_recv.at[n], device_id=partner, device_id_type=MESH)

    for r in range(2):

        @pl.when((row == r) & (owner != r))
        def _():
            for copy in own_away(r):
                copy.start()

        @pl.when((row == r) & (owner == r))
        def _():
            stays = [pltpu.make_async_copy(src, dst, own_send.at[2 + n]) for n, (src, dst) in enumerate(own_copies(r))]
            for copy in stays:
                copy.start()
            for copy in stays:
                copy.wait()
            for copy in own_away(1 - r):
                copy.wait_recv()

    for h in range(H):
        gather.first(h, 0)

    rows_i = lax.broadcasted_iota(jnp.int32, (64, 256), 0)
    const[0:64, :] = jnp.where(rows_i < 3, 1.0, 0.0).astype(BF)
    eye_r = lax.broadcasted_iota(jnp.int32, (128, 256), 0)
    eye_c = lax.broadcasted_iota(jnp.int32, (128, 256), 1)
    const[64:192, :] = jnp.where((eye_c == eye_r) | (eye_c == eye_r + 128), 1.0, 0.0).astype(BF)
    piece = lax.broadcasted_iota(jnp.int32, (64, 128), 0)
    fill = jnp.where(piece == 0, FILL_PARTS[0], jnp.where(piece == 1, FILL_PARTS[1], jnp.where(piece == 2, FILL_PARTS[2], 0.0)))
    for t in range(4):
        shut = jnp.where(mask_ref[pl.ds(row * 4 + t, 1), :] > 0, 0.0, 1.0)
        fill_rows[:, t * 128:(t + 1) * 128] = (fill * shut).astype(BF)
    for n, w_ref in enumerate((wq_ref, wk_ref, wv_ref, wg_ref, wo_ref)):
        weights[n * C:(n + 1) * C, :] = w_ref[...].T
    wt = weights[0:4 * C, :]

    def project(j, carry):
        r = jnp.dot(wt, normed[j], preferred_element_type=F32)
        q = (r[0:64] * (1.0 / math.sqrt(D))).astype(BF)
        k = r[64:128].astype(BF)
        v = r[128:192].astype(BF)
        g = jax.nn.sigmoid(r[192:256])
        for h in range(H):
            sl = slice(h * D, (h + 1) * D)
            keys_t[h, j] = k[sl]
            values[row, h, j] = v[sl]
            for ib in range(NIB):
                query[h, ib, j] = q[sl, ib * 128:(ib + 1) * 128]
                gate[h, ib, j] = g[sl, ib * 128:(ib + 1) * 128]
        return carry

    def turn_keys(n, carry):
        kt = keys_t[n // 4, pl.ds((n % 4) * 4, 4)].reshape(64, R)
        full = jnp.concatenate([kt, fill_rows[...]], axis=0)
        keys[row, n] = full.T
        return carry

    def kv_copies(h, r):
        for n, ref in enumerate((keys.at[r, pl.ds(h * 4, 4)], values.at[r, h])):
            yield pltpu.make_async_remote_copy(src_ref=ref, dst_ref=ref, send_sem=kv_send.at[h * 2 + n], recv_sem=kv_recv.at[h * 2 + n], device_id=partner, device_id_type=MESH)

    lax.fori_loop(0, 8, project, 0)
    gather.step1(0)
    lax.fori_loop(8, 16, project, 0)
    gather.step2(0)
    gather.step1(1)
    lax.fori_loop(0, 16, turn_keys, 0)
    for h in range(H):
        for copy in kv_copies(h, row):
            copy.start()
    gather.relay(0)
    gather.step2(1)

    logits[1] = jnp.zeros((2 * R, 256), F32)
    best[1] = jnp.zeros((1, 256), F32)

    @pl.loop(0, H * NIB)
    def _(n):
        h, ib = n // NIB, n % NIB

        @pl.when(ib == 0)
        def _():
            for copy in kv_copies(h, 1 - row):
                copy.wait_recv()
            gather.finish(h)

        @pl.when((ib == 0) & (h < H - 2))
        def _():
            gather.step1(h + 2)

        @pl.when((ib == 1) & (h < H - 1))
        def _():
            gather.relay(h + 1)

        @pl.when((ib == 2) & (h < H - 2))
        def _():
            gather.step2(h + 2)

        last = jnp.maximum(n - 1, 0)
        attend(h, ib, (last // NIB, last % NIB), bias_all, query, keys, values, gate, gated, const, bias_kt, logits, best)

    mix(7, H - 1, NIB - 1, values, gate, gated, logits, best)
    project_out(pair_ref, weights, gated, out_ref)

    @pl.loop(0, H)
    def _(h):
        for phase in range(3):
            gather.first(h, phase, "wait_send")
        gather.relay(h, "wait_send")
        for copy in kv_copies(h, row):
            copy.wait_send()

    for r in range(2):

        @pl.when((row == r) & (owner != r))
        def _():
            for copy in own_away(r):
                copy.wait_send()


def mix(p, h, ib, values, gate, gated, logits, best):
    total = jnp.zeros((1, 256), F32)
    acc = None
    for kh in range(2):
        e = jnp.exp2((logits[p % 2, kh * R:(kh + 1) * R, :] - best[p % 2]) * LOG2E)
        total = total + jnp.sum(e, axis=0, keepdims=True)
        v = jnp.concatenate([values[kh, h, 2 * p], values[kh, h, 2 * p + 1]], axis=0)
        o = jnp.dot(v, e.astype(BF), preferred_element_type=F32)
        acc = o if acc is None else acc + o
    scale = 1.0 / total
    gated[ib, 2 * p, h] = (gate[h, ib, 2 * p] * (acc[0:16, 0:128] * scale[:, 0:128])).astype(BF)
    gated[ib, 2 * p + 1, h] = (gate[h, ib, 2 * p + 1] * (acc[16:32, 128:256] * scale[:, 128:256])).astype(BF)


def attend(h, ib, before, bias_all, query, keys, values, gate, gated, const, bias_kt, logits, best):
    for t in range(8):
        part = 0 if t < 3 else 1 if t < 6 else 2
        z, y, tile = ib // 2, (ib % 2) * 2, t - PARTS[part][0]
        rows = []
        for n in range(8):
            pos = {"z": z, "y": y + n // 4, "x": n % 4}
            rows.append(bias_all[part][(h, *(pos[dim] for dim in reversed(ORDERS[part])), tile)])
        bias_kt[t * 128:(t + 1) * 128, :] = jnp.concatenate(rows, axis=0).T

    def score(p):
        group, odd = p // 2, p % 2
        zero = jnp.zeros((16, 128), BF)
        gap = jnp.zeros((16, 256), BF)
        left = jnp.concatenate([query[h, ib, 2 * p], zero], axis=1)
        right = jnp.concatenate([zero, query[h, ib, 2 * p + 1]], axis=1)
        top = [gap, gap, left, right] if odd else [left, right, gap, gap]
        rhs = jnp.concatenate(top + [const[...]], axis=0)
        high = None
        for kh in range(2):
            lhs = jnp.concatenate([keys[kh, h * 4 + group], bias_kt[kh * R:(kh + 1) * R, :]], axis=1)
            s = jnp.dot(lhs, rhs, preferred_element_type=F32)
            logits[p % 2, kh * R:(kh + 1) * R, :] = s
            m = jnp.max(s, axis=0, keepdims=True)
            high = m if high is None else jnp.maximum(high, m)
        best[p % 2] = high

    for p in range(8):
        score(p)
        mix((p + 7) % 8, *((h, ib) if p else before), values, gate, gated, logits, best)


def project_out(pair_ref, weights, gated, out_ref):
    wot = weights[4 * C:5 * C, :]

    def one(j, carry):
        g = jnp.concatenate([gated[ib, j].reshape(64, 128) for ib in range(NIB)], axis=1)
        update = jnp.dot(wot, g, preferred_element_type=F32)
        out_ref[j] = (pair_ref[j].astype(F32) + update).astype(BF)
        return carry

    lax.fori_loop(0, J, one, 0)


SCRATCH = dict(
    normed=((J, C, R), BF), bias_f32=((H, J, R), F32), bias_own=((H, 4, J, 128), BF), bias_a=((H, 2, 4, 4, 3, J, 128), BF), bias_b=((H, 4, 2, 4, 3, J, 128), BF), bias_c=((H, 4, 4, 2, 2, J, 128), BF),
    query=((H, NIB, J, D, 128), BF), keys_t=((H, J, D, R), BF), keys=((2, 16, R, 128), BF), values=((2, H, J, D, R), BF),
    gate=((H, NIB, J, D, 128), F32), gated=((NIB, J, H, D, 128), BF), const=((192, 256), BF), fill_rows=((64, R), BF), weights=((5 * C, C), BF),
    bias_kt=((2 * R, 128), BF), logits=((2, 2 * R, 256), F32), best=((2, 1, 256), F32))


def solution(mesh):
    def body(pair_tile, res_mask, ln_gamma, ln_beta, w_q, w_k, w_v, w_b, w_g, w_o):
        pair_t = jnp.transpose(pair_tile, (1, 2, 0))
        scratch = [pltpu.VMEM(shape, dtype) for shape, dtype in SCRATCH.values()]
        sems = [pltpu.SemaphoreType.DMA((n,)) for n in (H * 36, H * 36, 4, 2, 2 * H, 2 * H)]
        out_t = pl.pallas_call(
            kernel,
            out_shape=jax.ShapeDtypeStruct((J, C, R), BF),
            in_specs=[pl.BlockSpec(memory_space=pltpu.VMEM)] * 10,
            out_specs=pl.BlockSpec(memory_space=pltpu.VMEM),
            scratch_shapes=scratch + sems,
            compiler_params=pltpu.CompilerParams(collective_id=0, has_side_effects=True, vmem_limit_bytes=60 * 1024 * 1024),
        )(pair_t, res_mask.reshape(8, 128), ln_gamma.reshape(1, C), ln_beta.reshape(1, C), w_q, w_k, w_v, w_g, w_b.T, w_o)
        return jnp.transpose(out_t, (2, 0, 1))

    tile_spec = P(("data", "row"), "col", None)
    return jax.shard_map(body, mesh=mesh, in_specs=(tile_spec, P("data"), P(), P(), P(), P(), P(), P(), P(), P()), out_specs=tile_spec, check_vma=False)
```

```python
import functools
import math
import jax
import jax.numpy as jnp
from jax import lax
from jax.experimental import pallas as pl
from jax.experimental.pallas import tpu as pltpu
from jax.sharding import PartitionSpec as P

LN_EPS = 1e-5
LOG2E = math.log2(math.e)
FILL_PARTS = (-998244352.0, -1753088.0, -2560.0)
J, C, R, H, D = 16, 64, 512, 4, 16
NIB = 4
MESH = pl.DeviceIdType.MESH
BF, F32 = jnp.bfloat16, jnp.float32
PARTS = ((0, 3), (3, 3), (6, 2))
ORDERS = (("x", "y", "z"), ("y", "z", "x"), ("z", "x", "y"))


class Gather:
    def __init__(self, bias_own, bias_all, spare, send_sem, recv_sem, plane_send, plane_recv, own_send):
        self.own, self.bufs, self.spare, self.send_sem, self.recv_sem = bias_own, bias_all, spare, send_sem, recv_sem
        self.plane_sem, self.plane_recv, self.own_sem = plane_send, plane_recv, own_send
        self.col, self.row = lax.axis_index("col"), lax.axis_index("row")
        self.z, self.y, self.x = self.col // 16, (self.col // 4) % 4, self.col % 4
        self.turn = (self.z - 2 * self.row + 4) % 4
        self.owner = self.z // 2
        self.source = self.turn < 2

    def neighbour(self, dim, step):
        z, y, x = self.z, self.y, self.x
        if dim == "z":
            z = (z + step + 4) % 4
        elif dim == "y":
            y = (y + step + 4) % 4
        else:
            x = (x + step + 4) % 4
        return {"col": (z * 4 + y) * 4 + x, "row": self.row}

    def here(self, dim):
        return {"z": self.z % 2, "y": self.y, "x": self.x}[dim]

    def pieces(self, head, act):
        for r, own in enumerate((((0, 0, 0, 3), (3, 1, 0, 1)), ((0, 1, 1, 2), (2, 2, 0, 2)))):
            for tiles, part, lo, size in own:
                order, sem = ORDERS[part], head * 3 + part
                src = self.own.at[head, pl.ds(tiles, size)]
                dst = self.bufs[part].at[(head, *(self.here(dim) for dim in reversed(order)), pl.ds(lo, size))]

                def away(device, src=src, dst=dst, sem=sem, send=self.plane_sem):
                    return pltpu.make_async_remote_copy(src_ref=src, dst_ref=dst, send_sem=send.at[sem], recv_sem=self.plane_recv.at[sem], device_id=device, device_id_type=MESH)

                def start():
                    @pl.loop(1, 16)
                    def _(n):
                        at = {"z": self.z, "y": self.y, "x": self.x}
                        for dim, step in zip(order[:2], (n % 4, n // 4)):
                            at[dim] = (at[dim] + step) % 4
                        away({"col": (at["z"] * 4 + at["y"]) * 4 + at["x"], "row": self.owner}).start()

                def wait():
                    ref = self.spare.at[pl.ds(0, 15 * size)]
                    away({"row": 1 - self.row}, ref, ref).wait_send()

                def stay():
                    pltpu.make_async_copy(src, dst, self.plane_recv.at[sem]).start()

                def cross():
                    copy = away({"row": 1 - self.row}, send=self.own_sem)
                    copy.start() if act == "start" else copy.wait_send()

                pl.when(self.row == r)(start if act == "start" else wait)
                pl.when((self.row == r) & (self.owner != r))(cross)
                if act == "start":
                    pl.when((self.row == r) & (self.owner == r))(stay)

    def arrived(self, head):
        for part in range(3):
            ref = self.bufs[part].at[head, self.here(ORDERS[part][2])]
            wait = pltpu.make_async_remote_copy(src_ref=ref, dst_ref=ref, send_sem=self.own_sem.at[0], recv_sem=self.plane_recv.at[head * 3 + part], device_id={"row": 1 - self.row}, device_id_type=MESH).wait_recv
            pl.when(self.source)(wait) if part == 0 else wait()

    def copy(self, head, part, slot, value, half, step):
        order = ORDERS[part]
        middle = slice(None)
        if half is not None:
            size = 1 if order[1] == "z" else 2
            middle = pl.ds(half * size, size)
        ref = self.bufs[part].at[head, value, middle]
        sem = (head * 3 + part) * 4 + slot
        return pltpu.make_async_remote_copy(src_ref=ref, dst_ref=ref, send_sem=self.send_sem.at[sem], recv_sem=self.recv_sem.at[sem], device_id=self.neighbour(order[2], step), device_id_type=MESH)

    def first(self, head, act="start"):
        for part in range(3):

            def go():
                for slot, step in ((0, 1), (1, -1)):
                    getattr(self.copy(head, part, slot, self.here(ORDERS[part][2]), None, step), act)()

            pl.when(self.source)(go) if part == 0 else go()

    def relay(self, head, act="start"):
        for part in range(3):
            dim = ORDERS[part][2]
            if dim == "z":
                cases = ((0, 1, 1, 0, -1, 3), (1, 0, 0, 0, 1, 2), (2, 0, 1, 1, 1, 2), (3, 1, 0, 1, -1, 3))
                for turn, slot, value, half, step, out in cases:

                    @pl.when(self.turn == turn)
                    def _():
                        if act == "start":
                            self.copy(head, part, slot, value, None, 1).wait_recv()
                        getattr(self.copy(head, part, out, value, half, step), act)()

                continue
            for slot, back, half, step in ((0, 3, 0, 1), (1, 1, 1, -1)):
                value = (self.here(dim) + back) % 4
                if act == "start":
                    self.copy(head, part, slot, value, None, 1).wait_recv()
                getattr(self.copy(head, part, slot + 2, value, half, step), act)()

    def finish(self, head):
        for part in range(3):
            dim = ORDERS[part][2]
            if dim == "z":
                for turn, value, slots in ((2, 0, ((2, 0), (3, 1))), (3, 1, ((3, 0), (2, 1)))):

                    @pl.when(self.turn == turn)
                    def _():
                        for slot, half in slots:
                            self.copy(head, part, slot, value, half, 1).wait_recv()

                continue
            for slot, half in ((2, 0), (3, 1)):
                self.copy(head, part, slot, (self.here(dim) + 2) % 4, half, 1).wait_recv()

    def forward(self, head):
        self.arrived(head)
        self.first(head)


def kernel(pair_ref, mask_ref, gamma_ref, beta_ref, wq_ref, wk_ref, wv_ref, wg_ref, wbt_ref, wo_ref, out_ref,
           normed, bias_f32, bias_own, spare, bias_a, bias_b, bias_c, query, keys_t, keys, values, gate, gated, const, fill_rows, weights, bias_kt, logits, best,
           send_sem, recv_sem, plane_send, plane_recv, own_send, kv_send, kv_recv):
    row = lax.axis_index("row")
    bias_all = (bias_a, bias_b, bias_c)
    gather = Gather(bias_own, bias_all, spare, send_sem, recv_sem, plane_send, plane_recv, own_send)
    partner = {"row": 1 - row}

    barrier = pltpu.get_barrier_semaphore()
    pl.semaphore_signal(barrier, inc=1, device_id=partner, device_id_type=MESH)

    @pl.loop(1, 64)
    def _(n):
        dz, dy, dx = n // 16, n // 4 % 4, n % 4

        @pl.when((dz == 0) | (dy == 0) | (dx == 0))
        def _():
            col = ((gather.z + dz) % 4 * 4 + (gather.y + dy) % 4) * 4 + (gather.x + dx) % 4
            for r in range(2):
                pl.semaphore_signal(barrier, inc=1, device_id={"col": col, "row": r}, device_id_type=MESH)

    diag = lax.broadcasted_iota(jnp.int32, (C, C), 0) == lax.broadcasted_iota(jnp.int32, (C, C), 1)
    gamma = jnp.sum(jnp.where(diag, gamma_ref[...], 0.0), axis=1, keepdims=True)
    beta = jnp.sum(jnp.where(diag, beta_ref[...], 0.0), axis=1, keepdims=True)
    wbt = wbt_ref[...]
    for j in range(J):
        pair = pair_ref[j].astype(F32)
        mean = jnp.mean(pair, axis=0, keepdims=True)
        centred = pair - mean
        variance = jnp.mean(centred * centred, axis=0, keepdims=True)
        a = (centred * lax.rsqrt(variance + LN_EPS) * gamma + beta).astype(BF)
        normed[j] = a
        b = jnp.dot(wbt, a, preferred_element_type=F32)
        for h in range(H):
            bias_f32[h, j:j + 1, :] = b[h:h + 1, :]
    for h in range(H):
        for t in range(4):
            bias_own[h, t] = bias_f32[h, :, t * 128:(t + 1) * 128].astype(BF)

    pl.semaphore_wait(barrier, 73)

    gather.pieces(0, "start")
    gather.pieces(1, "start")

    rows_i = lax.broadcasted_iota(jnp.int32, (64, 256), 0)
    const[0:64, :] = jnp.where(rows_i < 3, 1.0, 0.0).astype(BF)
    eye_r = lax.broadcasted_iota(jnp.int32, (128, 256), 0)
    eye_c = lax.broadcasted_iota(jnp.int32, (128, 256), 1)
    const[64:192, :] = jnp.where((eye_c == eye_r) | (eye_c == eye_r + 128), 1.0, 0.0).astype(BF)
    piece = lax.broadcasted_iota(jnp.int32, (64, 128), 0)
    fill = jnp.where(piece == 0, FILL_PARTS[0], jnp.where(piece == 1, FILL_PARTS[1], jnp.where(piece == 2, FILL_PARTS[2], 0.0)))
    for t in range(4):
        shut = jnp.where(mask_ref[pl.ds(row * 4 + t, 1), :] > 0, 0.0, 1.0)
        fill_rows[:, t * 128:(t + 1) * 128] = (fill * shut).astype(BF)
    for n, w_ref in enumerate((wq_ref, wk_ref, wv_ref, wg_ref, wo_ref)):
        weights[n * C:(n + 1) * C, :] = w_ref[...].T
    wt = weights[0:4 * C, :]

    def project(j, carry):
        r = jnp.dot(wt, normed[j], preferred_element_type=F32)
        q = (r[0:64] * (1.0 / math.sqrt(D))).astype(BF)
        k = r[64:128].astype(BF)
        v = r[128:192].astype(BF)
        g = jax.nn.sigmoid(r[192:256])
        for h in range(H):
            sl = slice(h * D, (h + 1) * D)
            keys_t[h, j] = k[sl]
            values[row, h, j] = v[sl]
            for ib in range(NIB):
                query[h, ib, j] = q[sl, ib * 128:(ib + 1) * 128]
                gate[h, ib, j] = g[sl, ib * 128:(ib + 1) * 128]
        return carry

    def turn_keys(n, carry):
        kt = keys_t[n // 4, pl.ds((n % 4) * 4, 4)].reshape(64, R)
        full = jnp.concatenate([kt, fill_rows[...]], axis=0)
        keys[row, n] = full.T
        return carry

    def kv_copies(h, r):
        for n, ref in enumerate((keys.at[r, pl.ds(h * 4, 4)], values.at[r, h])):
            yield pltpu.make_async_remote_copy(src_ref=ref, dst_ref=ref, send_sem=kv_send.at[h * 2 + n], recv_sem=kv_recv.at[h * 2 + n], device_id=partner, device_id_type=MESH)

    lax.fori_loop(0, 16, project, 0)
    gather.forward(0)
    lax.fori_loop(0, 16, turn_keys, 0)
    for h in range(H):
        for copy in kv_copies(h, row):
            copy.start()
    gather.relay(0)
    gather.forward(1)
    gather.pieces(2, "start")
    schedule = ((1, gather.relay, 1), (2, gather.forward, 2), (3, lambda h: gather.pieces(h, "start"), 3), (5, gather.relay, 2), (7, gather.forward, 3), (10, gather.relay, 3))

    logits[1] = jnp.zeros((2 * R, 256), F32)
    best[1] = jnp.zeros((1, 256), F32)

    @pl.loop(0, H * NIB)
    def _(n):
        h, ib = n // NIB, n % NIB

        @pl.when(ib == 0)
        def _():
            for copy in kv_copies(h, 1 - row):
                copy.wait_recv()
            gather.finish(h)

        for unit, step, head in schedule:
            pl.when(n == unit)(functools.partial(step, head))

        last = jnp.maximum(n - 1, 0)
        attend(h, ib, (last // NIB, last % NIB), bias_all, query, keys, values, gate, gated, const, bias_kt, logits, best)

    mix(7, H - 1, NIB - 1, values, gate, gated, logits, best)
    project_out(pair_ref, weights, gated, out_ref)

    @pl.loop(0, H)
    def _(h):
        gather.pieces(h, "wait")
        gather.first(h, "wait_send")
        gather.relay(h, "wait_send")
        for copy in kv_copies(h, row):
            copy.wait_send()


def mix(p, h, ib, values, gate, gated, logits, best):
    total = jnp.zeros((1, 256), F32)
    acc = None
    for kh in range(2):
        e = jnp.exp2((logits[p % 2, kh * R:(kh + 1) * R, :] - best[p % 2]) * LOG2E)
        total = total + jnp.sum(e, axis=0, keepdims=True)
        v = jnp.concatenate([values[kh, h, 2 * p], values[kh, h, 2 * p + 1]], axis=0)
        o = jnp.dot(v, e.astype(BF), preferred_element_type=F32)
        acc = o if acc is None else acc + o
    scale = 1.0 / total
    gated[ib, 2 * p, h] = (gate[h, ib, 2 * p] * (acc[0:16, 0:128] * scale[:, 0:128])).astype(BF)
    gated[ib, 2 * p + 1, h] = (gate[h, ib, 2 * p + 1] * (acc[16:32, 128:256] * scale[:, 128:256])).astype(BF)


def attend(h, ib, before, bias_all, query, keys, values, gate, gated, const, bias_kt, logits, best):
    for t in range(8):
        part = 0 if t < 3 else 1 if t < 6 else 2
        z, y, tile = ib // 2, (ib % 2) * 2, t - PARTS[part][0]
        rows = []
        for n in range(8):
            pos = {"z": z, "y": y + n // 4, "x": n % 4}
            rows.append(bias_all[part][(h, *(pos[dim] for dim in reversed(ORDERS[part])), tile)])
        bias_kt[t * 128:(t + 1) * 128, :] = jnp.concatenate(rows, axis=0).T

    def score(p):
        group, odd = p // 2, p % 2
        zero = jnp.zeros((16, 128), BF)
        gap = jnp.zeros((16, 256), BF)
        left = jnp.concatenate([query[h, ib, 2 * p], zero], axis=1)
        right = jnp.concatenate([zero, query[h, ib, 2 * p + 1]], axis=1)
        top = [gap, gap, left, right] if odd else [left, right, gap, gap]
        rhs = jnp.concatenate(top + [const[...]], axis=0)
        high = None
        for kh in range(2):
            lhs = jnp.concatenate([keys[kh, h * 4 + group], bias_kt[kh * R:(kh + 1) * R, :]], axis=1)
            s = jnp.dot(lhs, rhs, preferred_element_type=F32)
            logits[p % 2, kh * R:(kh + 1) * R, :] = s
            m = jnp.max(s, axis=0, keepdims=True)
            high = m if high is None else jnp.maximum(high, m)
        best[p % 2] = high

    for p in range(8):
        score(p)
        mix((p + 7) % 8, *((h, ib) if p else before), values, gate, gated, logits, best)


def project_out(pair_ref, weights, gated, out_ref):
    wot = weights[4 * C:5 * C, :]

    def one(j, carry):
        g = jnp.concatenate([gated[ib, j].reshape(64, 128) for ib in range(NIB)], axis=1)
        update = jnp.dot(wot, g, preferred_element_type=F32)
        out_ref[j] = (pair_ref[j].astype(F32) + update).astype(BF)
        return carry

    lax.fori_loop(0, J, one, 0)


SCRATCH = dict(
    normed=((J, C, R), BF), bias_f32=((H, J, R), F32), bias_own=((H, 4, J, 128), BF), spare=((45, J, 128), BF), bias_a=((H, 2, 4, 4, 3, J, 128), BF), bias_b=((H, 4, 2, 4, 3, J, 128), BF), bias_c=((H, 4, 4, 2, 2, J, 128), BF),
    query=((H, NIB, J, D, 128), BF), keys_t=((H, J, D, R), BF), keys=((2, 16, R, 128), BF), values=((2, H, J, D, R), BF),
    gate=((H, NIB, J, D, 128), F32), gated=((NIB, J, H, D, 128), BF), const=((192, 256), BF), fill_rows=((64, R), BF), weights=((5 * C, C), BF),
    bias_kt=((2 * R, 128), BF), logits=((2, 2 * R, 256), F32), best=((2, 1, 256), F32))


def solution(mesh):
    def body(pair_tile, res_mask, ln_gamma, ln_beta, w_q, w_k, w_v, w_b, w_g, w_o):
        pair_t = jnp.transpose(pair_tile, (1, 2, 0))
        scratch = [pltpu.VMEM(shape, dtype) for shape, dtype in SCRATCH.values()]
        sems = [pltpu.SemaphoreType.DMA((n,)) for n in (H * 12, H * 12, H * 3, H * 3, H * 3, 2 * H, 2 * H)]
        out_t = pl.pallas_call(
            kernel,
            out_shape=jax.ShapeDtypeStruct((J, C, R), BF),
            in_specs=[pl.BlockSpec(memory_space=pltpu.VMEM)] * 10,
            out_specs=pl.BlockSpec(memory_space=pltpu.VMEM),
            scratch_shapes=scratch + sems,
            compiler_params=pltpu.CompilerParams(collective_id=0, has_side_effects=True, vmem_limit_bytes=60 * 1024 * 1024),
        )(pair_t, res_mask.reshape(8, 128), ln_gamma.reshape(1, C), ln_beta.reshape(1, C), w_q, w_k, w_v, w_g, w_b.T, w_o)
        return jnp.transpose(out_t, (2, 0, 1))

    tile_spec = P(("data", "row"), "col", None)
    return jax.shard_map(body, mesh=mesh, in_specs=(tile_spec, P("data"), P(), P(), P(), P(), P(), P(), P(), P()), out_specs=tile_spec, check_vma=False)
```

```python
import functools
import math
import jax
import jax.numpy as jnp
from jax import lax
from jax.experimental import pallas as pl
from jax.experimental.pallas import tpu as pltpu
from jax.sharding import PartitionSpec as P

LN_EPS = 1e-5
LOG2E = math.log2(math.e)
FILL_PARTS = (-998244352.0, -1753088.0, -2560.0)
J, C, R, H, D = 16, 64, 512, 4, 16
NIB = 4
MESH = pl.DeviceIdType.MESH
BF, F32 = jnp.bfloat16, jnp.float32
PARTS = ((0, 3), (3, 3), (6, 2))
ORDERS = (("x", "y", "z"), ("y", "z", "x"), ("z", "x", "y"))


class Gather:
    def __init__(self, bias_own, bias_all, spare, send_sem, recv_sem, plane_send, plane_recv, own_send):
        self.own, self.bufs, self.spare, self.send_sem, self.recv_sem = bias_own, bias_all, spare, send_sem, recv_sem
        self.plane_sem, self.plane_recv, self.own_sem = plane_send, plane_recv, own_send
        self.col, self.row = lax.axis_index("col"), lax.axis_index("row")
        self.z, self.y, self.x = self.col // 16, (self.col // 4) % 4, self.col % 4
        self.turn = (self.z - 2 * self.row + 4) % 4
        self.owner = self.z // 2
        self.source = self.turn < 2

    def neighbour(self, dim, step):
        z, y, x = self.z, self.y, self.x
        if dim == "z":
            z = (z + step + 4) % 4
        elif dim == "y":
            y = (y + step + 4) % 4
        else:
            x = (x + step + 4) % 4
        return {"col": (z * 4 + y) * 4 + x, "row": self.row}

    def here(self, dim):
        return {"z": self.z % 2, "y": self.y, "x": self.x}[dim]

    def pieces(self, head, act):
        for r, own in enumerate((((0, 0, 0, 3), (3, 1, 0, 1)), ((0, 1, 1, 2), (2, 2, 0, 2)))):
            for tiles, part, lo, size in own:
                order, sem = ORDERS[part], head * 3 + part
                src = self.own.at[head, pl.ds(tiles, size)]
                dst = self.bufs[part].at[(head, *(self.here(dim) for dim in reversed(order)), pl.ds(lo, size))]

                def away(device, src=src, dst=dst, sem=sem, send=self.plane_sem):
                    return pltpu.make_async_remote_copy(src_ref=src, dst_ref=dst, send_sem=send.at[sem], recv_sem=self.plane_recv.at[sem], device_id=device, device_id_type=MESH)

                def start():
                    @pl.loop(1, 16)
                    def _(n):
                        at = {"z": self.z, "y": self.y, "x": self.x}
                        for dim, step in zip(order[:2], (n % 4, n // 4)):
                            at[dim] = (at[dim] + step) % 4
                        away({"col": (at["z"] * 4 + at["y"]) * 4 + at["x"], "row": self.owner}).start()

                def wait():
                    ref = self.spare.at[pl.ds(0, 15 * size)]
                    away({"row": 1 - self.row}, ref, ref).wait_send()

                def stay():
                    pltpu.make_async_copy(src, dst, self.plane_recv.at[sem]).start()

                def cross():
                    copy = away({"row": 1 - self.row}, send=self.own_sem)
                    copy.start() if act == "start" else copy.wait_send()

                pl.when(self.row == r)(start if act == "start" else wait)
                pl.when((self.row == r) & (self.owner != r))(cross)
                if act == "start":
                    pl.when((self.row == r) & (self.owner == r))(stay)

    def arrived(self, head):
        for part in range(3):
            ref = self.bufs[part].at[head, self.here(ORDERS[part][2])]
            wait = pltpu.make_async_remote_copy(src_ref=ref, dst_ref=ref, send_sem=self.own_sem.at[0], recv_sem=self.plane_recv.at[head * 3 + part], device_id={"row": 1 - self.row}, device_id_type=MESH).wait_recv
            pl.when(self.source)(wait) if part == 0 else wait()

    def copy(self, head, part, slot, value, half, step):
        order = ORDERS[part]
        middle = slice(None)
        if half is not None:
            size = 1 if order[1] == "z" else 2
            middle = pl.ds(half * size, size)
        ref = self.bufs[part].at[head, value, middle]
        sem = (head * 3 + part) * 4 + slot
        return pltpu.make_async_remote_copy(src_ref=ref, dst_ref=ref, send_sem=self.send_sem.at[sem], recv_sem=self.recv_sem.at[sem], device_id=self.neighbour(order[2], step), device_id_type=MESH)

    def first(self, head, act="start"):
        for part in range(3):

            def go():
                for slot, step in ((0, 1), (1, -1)):
                    getattr(self.copy(head, part, slot, self.here(ORDERS[part][2]), None, step), act)()

            pl.when(self.source)(go) if part == 0 else go()

    def relay(self, head, act="start"):
        for part in range(3):
            dim = ORDERS[part][2]
            if dim == "z":
                cases = ((0, 1, 1, 0, -1, 3), (1, 0, 0, 0, 1, 2), (2, 0, 1, 1, 1, 2), (3, 1, 0, 1, -1, 3))
                for turn, slot, value, half, step, out in cases:

                    @pl.when(self.turn == turn)
                    def _():
                        if act == "start":
                            self.copy(head, part, slot, value, None, 1).wait_recv()
                        getattr(self.copy(head, part, out, value, half, step), act)()

                continue
            for slot, back, half, step in ((0, 3, 0, 1), (1, 1, 1, -1)):
                value = (self.here(dim) + back) % 4
                if act == "start":
                    self.copy(head, part, slot, value, None, 1).wait_recv()
                getattr(self.copy(head, part, slot + 2, value, half, step), act)()

    def finish(self, head):
        for part in range(3):
            dim = ORDERS[part][2]
            if dim == "z":
                for turn, value, slots in ((2, 0, ((2, 0), (3, 1))), (3, 1, ((3, 0), (2, 1)))):

                    @pl.when(self.turn == turn)
                    def _():
                        for slot, half in slots:
                            self.copy(head, part, slot, value, half, 1).wait_recv()

                continue
            for slot, half in ((2, 0), (3, 1)):
                self.copy(head, part, slot, (self.here(dim) + 2) % 4, half, 1).wait_recv()

    def forward(self, head):
        self.arrived(head)
        self.first(head)


def kernel(pair_ref, mask_ref, gamma_ref, beta_ref, wq_ref, wk_ref, wv_ref, wg_ref, wbt_ref, wo_ref, out_ref,
           normed, bias_f32, bias_own, spare, bias_a, bias_b, bias_c, query, keys_t, keys, values, gate, gated, const, fill_rows, weights, bias_kt, logits, best,
           send_sem, recv_sem, plane_send, plane_recv, own_send, kv_send, kv_recv):
    row = lax.axis_index("row")
    bias_all = (bias_a, bias_b, bias_c)
    gather = Gather(bias_own, bias_all, spare, send_sem, recv_sem, plane_send, plane_recv, own_send)
    partner = {"row": 1 - row}

    barrier = pltpu.get_barrier_semaphore()
    pl.semaphore_signal(barrier, inc=1, device_id=partner, device_id_type=MESH)

    @pl.loop(1, 64)
    def _(n):
        dz, dy, dx = n // 16, n // 4 % 4, n % 4

        @pl.when((dz == 0) | (dy == 0) | (dx == 0))
        def _():
            col = ((gather.z + dz) % 4 * 4 + (gather.y + dy) % 4) * 4 + (gather.x + dx) % 4
            for r in range(2):
                pl.semaphore_signal(barrier, inc=1, device_id={"col": col, "row": r}, device_id_type=MESH)

    diag = lax.broadcasted_iota(jnp.int32, (C, C), 0) == lax.broadcasted_iota(jnp.int32, (C, C), 1)
    gamma = jnp.sum(jnp.where(diag, gamma_ref[...], 0.0), axis=1, keepdims=True)
    beta = jnp.sum(jnp.where(diag, beta_ref[...], 0.0), axis=1, keepdims=True)
    wbt = wbt_ref[...]
    for j in range(J):
        pair = pair_ref[j].astype(F32)
        mean = jnp.mean(pair, axis=0, keepdims=True)
        centred = pair - mean
        variance = jnp.mean(centred * centred, axis=0, keepdims=True)
        a = (centred * lax.rsqrt(variance + LN_EPS) * gamma + beta).astype(BF)
        normed[j] = a
        b = jnp.dot(wbt, a, preferred_element_type=F32)
        for h in range(H):
            bias_f32[h, j:j + 1, :] = b[h:h + 1, :]
    for h in range(H):
        for t in range(4):
            bias_own[h, t] = bias_f32[h, :, t * 128:(t + 1) * 128].astype(BF)

    pl.semaphore_wait(barrier, 73)

    gather.pieces(0, "start")

    rows_i = lax.broadcasted_iota(jnp.int32, (64, 256), 0)
    const[0:64, :] = jnp.where(rows_i < 3, 1.0, 0.0).astype(BF)
    eye_r = lax.broadcasted_iota(jnp.int32, (128, 256), 0)
    eye_c = lax.broadcasted_iota(jnp.int32, (128, 256), 1)
    const[64:192, :] = jnp.where((eye_c == eye_r) | (eye_c == eye_r + 128), 1.0, 0.0).astype(BF)
    piece = lax.broadcasted_iota(jnp.int32, (64, 128), 0)
    fill = jnp.where(piece == 0, FILL_PARTS[0], jnp.where(piece == 1, FILL_PARTS[1], jnp.where(piece == 2, FILL_PARTS[2], 0.0)))
    for t in range(4):
        shut = jnp.where(mask_ref[pl.ds(row * 4 + t, 1), :] > 0, 0.0, 1.0)
        fill_rows[:, t * 128:(t + 1) * 128] = (fill * shut).astype(BF)
    for n, w_ref in enumerate((wq_ref, wk_ref, wv_ref, wg_ref, wo_ref)):
        weights[n * C:(n + 1) * C, :] = w_ref[...].T
    wt = weights[0:4 * C, :]

    def project(j, carry):
        r = jnp.dot(wt, normed[j], preferred_element_type=F32)
        q = (r[0:64] * (1.0 / math.sqrt(D))).astype(BF)
        k = r[64:128].astype(BF)
        v = r[128:192].astype(BF)
        g = jax.nn.sigmoid(r[192:256])
        for h in range(H):
            sl = slice(h * D, (h + 1) * D)
            keys_t[h, j] = k[sl]
            values[row, h, j] = v[sl]
            for ib in range(NIB):
                query[h, ib, j] = q[sl, ib * 128:(ib + 1) * 128]
                gate[h, ib, j] = g[sl, ib * 128:(ib + 1) * 128]
        return carry

    def turn_keys(n, carry):
        kt = keys_t[n // 4, pl.ds((n % 4) * 4, 4)].reshape(64, R)
        full = jnp.concatenate([kt, fill_rows[...]], axis=0)
        keys[row, n] = full.T
        return carry

    def kv_copies(h, r):
        for n, ref in enumerate((keys.at[r, pl.ds(h * 4, 4)], values.at[r, h])):
            yield pltpu.make_async_remote_copy(src_ref=ref, dst_ref=ref, send_sem=kv_send.at[h * 2 + n], recv_sem=kv_recv.at[h * 2 + n], device_id=partner, device_id_type=MESH)

    lax.fori_loop(0, 16, project, 0)
    def kv_start(h):
        for copy in kv_copies(h, row):
            copy.start()

    def scatter(h):
        gather.pieces(h, "start")

    gather.forward(0)
    scatter(1)
    lax.fori_loop(0, 16, turn_keys, 0)
    kv_start(0)
    gather.relay(0)
    gather.forward(1)
    scatter(2)
    schedule = (
        (0, kv_start, 1), (1, gather.relay, 1), (1, scatter, 3), (1, kv_start, 2), (2, gather.forward, 2), (2, kv_start, 3),
        (5, gather.relay, 2), (5, gather.forward, 3), (8, gather.relay, 3))

    logits[1] = jnp.zeros((2 * R, 256), F32)
    best[1] = jnp.zeros((1, 256), F32)

    @pl.loop(0, H * NIB)
    def _(n):
        h, ib = n // NIB, n % NIB

        @pl.when(ib == 0)
        def _():
            for copy in kv_copies(h, 1 - row):
                copy.wait_recv()
            gather.finish(h)

        for unit, step, head in schedule:
            pl.when(n == unit)(functools.partial(step, head))

        last = jnp.maximum(n - 1, 0)
        attend(h, ib, (last // NIB, last % NIB), bias_all, query, keys, values, gate, gated, const, bias_kt, logits, best)

    mix(7, H - 1, NIB - 1, values, gate, gated, logits, best)
    project_out(pair_ref, weights, gated, out_ref)

    @pl.loop(0, H)
    def _(h):
        gather.pieces(h, "wait")
        gather.first(h, "wait_send")
        gather.relay(h, "wait_send")
        for copy in kv_copies(h, row):
            copy.wait_send()


def mix(p, h, ib, values, gate, gated, logits, best):
    total = jnp.zeros((1, 256), F32)
    acc = None
    for q in range(4):
        e = jnp.exp2((logits[p % 2, q * 256:q * 256 + 256, :] - best[p % 2]) * LOG2E)
        total = total + jnp.sum(e, axis=0, keepdims=True)
        vs = slice((q % 2) * 256, (q % 2) * 256 + 256)
        v = jnp.concatenate([values[q // 2, h, 2 * p, :, vs], values[q // 2, h, 2 * p + 1, :, vs]], axis=0)
        o = jnp.dot(v, e.astype(BF), preferred_element_type=F32)
        acc = o if acc is None else acc + o
    scale = 1.0 / total
    gated[ib, 2 * p, h] = (gate[h, ib, 2 * p] * (acc[0:16, 0:128] * scale[:, 0:128])).astype(BF)
    gated[ib, 2 * p + 1, h] = (gate[h, ib, 2 * p + 1] * (acc[16:32, 128:256] * scale[:, 128:256])).astype(BF)


def attend(h, ib, before, bias_all, query, keys, values, gate, gated, const, bias_kt, logits, best):
    for t in range(8):
        part = 0 if t < 3 else 1 if t < 6 else 2
        z, y, tile = ib // 2, (ib % 2) * 2, t - PARTS[part][0]
        rows = []
        for n in range(8):
            pos = {"z": z, "y": y + n // 4, "x": n % 4}
            rows.append(bias_all[part][(h, *(pos[dim] for dim in reversed(ORDERS[part])), tile)])
        bias_kt[t * 128:(t + 1) * 128, :] = jnp.concatenate(rows, axis=0).T

    def score(p):
        group, odd = p // 2, p % 2
        zero = jnp.zeros((16, 128), BF)
        gap = jnp.zeros((16, 256), BF)
        left = jnp.concatenate([query[h, ib, 2 * p], zero], axis=1)
        right = jnp.concatenate([zero, query[h, ib, 2 * p + 1]], axis=1)
        top = [gap, gap, left, right] if odd else [left, right, gap, gap]
        rhs = jnp.concatenate(top + [const[...]], axis=0)
        high = None
        for q in range(4):
            rs = slice(q * 256, q * 256 + 256)
            lhs = jnp.concatenate([keys[q // 2, h * 4 + group, (q % 2) * 256:(q % 2) * 256 + 256, :], bias_kt[rs, :]], axis=1)
            s = jnp.dot(lhs, rhs, preferred_element_type=F32)
            logits[p % 2, rs, :] = s
            m = jnp.max(s, axis=0, keepdims=True)
            high = m if high is None else jnp.maximum(high, m)
        best[p % 2] = high

    for p in range(8):
        score(p)
        mix((p + 7) % 8, *((h, ib) if p else before), values, gate, gated, logits, best)


def project_out(pair_ref, weights, gated, out_ref):
    wot = weights[4 * C:5 * C, :]

    def one(j, carry):
        g = jnp.concatenate([gated[ib, j].reshape(64, 128) for ib in range(NIB)], axis=1)
        update = jnp.dot(wot, g, preferred_element_type=F32)
        out_ref[j] = (pair_ref[j].astype(F32) + update).astype(BF)
        return carry

    lax.fori_loop(0, J, one, 0)


SCRATCH = dict(
    normed=((J, C, R), BF), bias_f32=((H, J, R), F32), bias_own=((H, 4, J, 128), BF), spare=((45, J, 128), BF), bias_a=((H, 2, 4, 4, 3, J, 128), BF), bias_b=((H, 4, 2, 4, 3, J, 128), BF), bias_c=((H, 4, 4, 2, 2, J, 128), BF),
    query=((H, NIB, J, D, 128), BF), keys_t=((H, J, D, R), BF), keys=((2, 16, R, 128), BF), values=((2, H, J, D, R), BF),
    gate=((H, NIB, J, D, 128), F32), gated=((NIB, J, H, D, 128), BF), const=((192, 256), BF), fill_rows=((64, R), BF), weights=((5 * C, C), BF),
    bias_kt=((2 * R, 128), BF), logits=((2, 2 * R, 256), F32), best=((2, 1, 256), F32))


def solution(mesh):
    def body(pair_tile, res_mask, ln_gamma, ln_beta, w_q, w_k, w_v, w_b, w_g, w_o):
        pair_t = jnp.transpose(pair_tile, (1, 2, 0))
        scratch = [pltpu.VMEM(shape, dtype) for shape, dtype in SCRATCH.values()]
        sems = [pltpu.SemaphoreType.DMA((n,)) for n in (H * 12, H * 12, H * 3, H * 3, H * 3, 2 * H, 2 * H)]
        out_t = pl.pallas_call(
            kernel,
            out_shape=jax.ShapeDtypeStruct((J, C, R), BF),
            in_specs=[pl.BlockSpec(memory_space=pltpu.VMEM)] * 10,
            out_specs=pl.BlockSpec(memory_space=pltpu.VMEM),
            scratch_shapes=scratch + sems,
            compiler_params=pltpu.CompilerParams(collective_id=0, has_side_effects=True, vmem_limit_bytes=60 * 1024 * 1024),
        )(pair_t, res_mask.reshape(8, 128), ln_gamma.reshape(1, C), ln_beta.reshape(1, C), w_q, w_k, w_v, w_g, w_b.T, w_o)
        return jnp.transpose(out_t, (2, 0, 1))

    tile_spec = P(("data", "row"), "col", None)
    return jax.shard_map(body, mesh=mesh, in_specs=(tile_spec, P("data"), P(), P(), P(), P(), P(), P(), P(), P()), out_specs=tile_spec, check_vma=False)
```

```python
import functools
import math
import jax
import jax.numpy as jnp
from jax import lax
from jax.experimental import pallas as pl
from jax.experimental.pallas import tpu as pltpu
from jax.sharding import PartitionSpec as P

LN_EPS = 1e-5
LOG2E = math.log2(math.e)
FILL_PARTS = (-998244352.0, -1753088.0, -2560.0)
J, C, R, H, D = 16, 64, 512, 4, 16
NIB = 4
MESH = pl.DeviceIdType.MESH
BF, F32 = jnp.bfloat16, jnp.float32
PARTS = ((0, 3), (3, 3), (6, 2))
ORDERS = (("x", "y", "z"), ("y", "z", "x"), ("z", "x", "y"))


class Gather:
    def __init__(self, bias_own, bias_all, spare, send_sem, recv_sem, plane_send, plane_recv, own_send):
        self.own, self.bufs, self.spare, self.send_sem, self.recv_sem = bias_own, bias_all, spare, send_sem, recv_sem
        self.plane_sem, self.plane_recv, self.own_sem = plane_send, plane_recv, own_send
        self.col, self.row = lax.axis_index("col"), lax.axis_index("row")
        self.z, self.y, self.x = self.col // 16, (self.col // 4) % 4, self.col % 4
        self.turn = (self.z - 2 * self.row + 4) % 4
        self.owner = self.z // 2
        self.source = self.turn < 2

    def neighbour(self, dim, step):
        z, y, x = self.z, self.y, self.x
        if dim == "z":
            z = (z + step + 4) % 4
        elif dim == "y":
            y = (y + step + 4) % 4
        else:
            x = (x + step + 4) % 4
        return {"col": (z * 4 + y) * 4 + x, "row": self.row}

    def here(self, dim):
        return {"z": self.z % 2, "y": self.y, "x": self.x}[dim]

    def pieces(self, head, act):
        for r, own in enumerate((((0, 0, 0, 3), (3, 1, 0, 1)), ((0, 1, 1, 2), (2, 2, 0, 2)))):
            for tiles, part, lo, size in own:
                order, sem = ORDERS[part], head * 3 + part
                src = self.own.at[head, pl.ds(tiles, size)]
                dst = self.bufs[part].at[(head, *(self.here(dim) for dim in reversed(order)), pl.ds(lo, size))]

                def away(device, src=src, dst=dst, sem=sem, send=self.plane_sem):
                    return pltpu.make_async_remote_copy(src_ref=src, dst_ref=dst, send_sem=send.at[sem], recv_sem=self.plane_recv.at[sem], device_id=device, device_id_type=MESH)

                def start():
                    @pl.loop(1, 16)
                    def _(n):
                        at = {"z": self.z, "y": self.y, "x": self.x}
                        for dim, step in zip(order[:2], (n % 4, n // 4)):
                            at[dim] = (at[dim] + step) % 4
                        away({"col": (at["z"] * 4 + at["y"]) * 4 + at["x"], "row": self.owner}).start()

                def wait():
                    ref = self.spare.at[pl.ds(0, 15 * size)]
                    away({"row": 1 - self.row}, ref, ref).wait_send()

                def stay():
                    pltpu.make_async_copy(src, dst, self.plane_recv.at[sem]).start()

                def cross():
                    copy = away({"row": 1 - self.row}, send=self.own_sem)
                    copy.start() if act == "start" else copy.wait_send()

                pl.when(self.row == r)(start if act == "start" else wait)
                pl.when((self.row == r) & (self.owner != r))(cross)
                if act == "start":
                    pl.when((self.row == r) & (self.owner == r))(stay)

    def arrived(self, head):
        for part in range(3):
            ref = self.bufs[part].at[head, self.here(ORDERS[part][2])]
            wait = pltpu.make_async_remote_copy(src_ref=ref, dst_ref=ref, send_sem=self.own_sem.at[0], recv_sem=self.plane_recv.at[head * 3 + part], device_id={"row": 1 - self.row}, device_id_type=MESH).wait_recv
            pl.when(self.source)(wait) if part == 0 else wait()

    def copy(self, head, part, slot, value, half, step):
        order = ORDERS[part]
        middle = slice(None)
        if half is not None:
            size = 1 if order[1] == "z" else 2
            middle = pl.ds(half * size, size)
        ref = self.bufs[part].at[head, value, middle]
        sem = (head * 3 + part) * 4 + slot
        return pltpu.make_async_remote_copy(src_ref=ref, dst_ref=ref, send_sem=self.send_sem.at[sem], recv_sem=self.recv_sem.at[sem], device_id=self.neighbour(order[2], step), device_id_type=MESH)

    def first(self, head, act="start"):
        for part in range(3):

            def go():
                for slot, step in ((0, 1), (1, -1)):
                    getattr(self.copy(head, part, slot, self.here(ORDERS[part][2]), None, step), act)()

            pl.when(self.source)(go) if part == 0 else go()

    def relay(self, head, act="start"):
        for part in range(3):
            dim = ORDERS[part][2]
            if dim == "z":
                cases = ((0, 1, 1, 0, -1, 3), (1, 0, 0, 0, 1, 2), (2, 0, 1, 1, 1, 2), (3, 1, 0, 1, -1, 3))
                for turn, slot, value, half, step, out in cases:

                    @pl.when(self.turn == turn)
                    def _():
                        if act == "start":
                            self.copy(head, part, slot, value, None, 1).wait_recv()
                        getattr(self.copy(head, part, out, value, half, step), act)()

                continue
            for slot, back, half, step in ((0, 3, 0, 1), (1, 1, 1, -1)):
                value = (self.here(dim) + back) % 4
                if act == "start":
                    self.copy(head, part, slot, value, None, 1).wait_recv()
                getattr(self.copy(head, part, slot + 2, value, half, step), act)()

    def finish(self, head):
        for part in range(3):
            dim = ORDERS[part][2]
            if dim == "z":
                for turn, value, slots in ((2, 0, ((2, 0), (3, 1))), (3, 1, ((3, 0), (2, 1)))):

                    @pl.when(self.turn == turn)
                    def _():
                        for slot, half in slots:
                            self.copy(head, part, slot, value, half, 1).wait_recv()

                continue
            for slot, half in ((2, 0), (3, 1)):
                self.copy(head, part, slot, (self.here(dim) + 2) % 4, half, 1).wait_recv()

    def forward(self, head):
        self.arrived(head)
        self.first(head)


def kernel(pair_ref, mask_ref, gamma_ref, beta_ref, wq_ref, wk_ref, wv_ref, wg_ref, wbt_ref, wo_ref, out_ref,
           normed, bias_f32, bias_own, spare, bias_a, bias_b, bias_c, query, keys_t, keys, values, gate, gated, const, fill_rows, weights, bias_kt, logits, best,
           send_sem, recv_sem, plane_send, plane_recv, own_send, kv_send, kv_recv):
    row = lax.axis_index("row")
    bias_all = (bias_a, bias_b, bias_c)
    gather = Gather(bias_own, bias_all, spare, send_sem, recv_sem, plane_send, plane_recv, own_send)
    partner = {"row": 1 - row}

    barrier = pltpu.get_barrier_semaphore()
    pl.semaphore_signal(barrier, inc=1, device_id=partner, device_id_type=MESH)

    @pl.loop(1, 64)
    def _(n):
        dz, dy, dx = n // 16, n // 4 % 4, n % 4

        @pl.when((dz == 0) | (dy == 0) | (dx == 0))
        def _():
            col = ((gather.z + dz) % 4 * 4 + (gather.y + dy) % 4) * 4 + (gather.x + dx) % 4
            for r in range(2):
                pl.semaphore_signal(barrier, inc=1, device_id={"col": col, "row": r}, device_id_type=MESH)

    diag = lax.broadcasted_iota(jnp.int32, (C, C), 0) == lax.broadcasted_iota(jnp.int32, (C, C), 1)
    gamma = jnp.sum(jnp.where(diag, gamma_ref[...], 0.0), axis=1, keepdims=True)
    beta = jnp.sum(jnp.where(diag, beta_ref[...], 0.0), axis=1, keepdims=True)
    wbt = wbt_ref[...]
    for j in range(J):
        pair = pair_ref[j].astype(F32)
        mean = jnp.mean(pair, axis=0, keepdims=True)
        centred = pair - mean
        variance = jnp.mean(centred * centred, axis=0, keepdims=True)
        a = (centred * lax.rsqrt(variance + LN_EPS) * gamma + beta).astype(BF)
        normed[j] = a
        b = jnp.dot(wbt, a, preferred_element_type=F32)
        for h in range(H):
            bias_f32[h, j:j + 1, :] = b[h:h + 1, :]
    for h in range(H):
        for t in range(4):
            bias_own[h, t] = bias_f32[h, :, t * 128:(t + 1) * 128].astype(BF)

    pl.semaphore_wait(barrier, 73)

    gather.pieces(0, "start")

    rows_i = lax.broadcasted_iota(jnp.int32, (64, 256), 0)
    const[0:64, :] = jnp.where(rows_i < 3, 1.0, 0.0).astype(BF)
    eye_r = lax.broadcasted_iota(jnp.int32, (128, 256), 0)
    eye_c = lax.broadcasted_iota(jnp.int32, (128, 256), 1)
    const[64:192, :] = jnp.where((eye_c == eye_r) | (eye_c == eye_r + 128), 1.0, 0.0).astype(BF)
    piece = lax.broadcasted_iota(jnp.int32, (64, 128), 0)
    fill = jnp.where(piece == 0, FILL_PARTS[0], jnp.where(piece == 1, FILL_PARTS[1], jnp.where(piece == 2, FILL_PARTS[2], 0.0)))
    for t in range(4):
        shut = jnp.where(mask_ref[pl.ds(row * 4 + t, 1), :] > 0, 0.0, 1.0)
        fill_rows[:, t * 128:(t + 1) * 128] = (fill * shut).astype(BF)
    for n, w_ref in enumerate((wq_ref, wk_ref, wv_ref, wg_ref, wo_ref)):
        weights[n * C:(n + 1) * C, :] = w_ref[...].T
    wt = weights[0:4 * C, :]

    def project(j, carry):
        r = jnp.dot(wt, normed[j], preferred_element_type=F32)
        q = (r[0:64] * (1.0 / math.sqrt(D))).astype(BF)
        k = r[64:128].astype(BF)
        v = r[128:192].astype(BF)
        g = jax.nn.sigmoid(r[192:256])
        for h in range(H):
            sl = slice(h * D, (h + 1) * D)
            keys_t[h, j] = k[sl]
            values[row, h, j] = v[sl]
            for ib in range(NIB):
                query[h, ib, j] = q[sl, ib * 128:(ib + 1) * 128]
                gate[h, ib, j] = g[sl, ib * 128:(ib + 1) * 128]
        return carry

    def turn_keys(n, carry):
        kt = keys_t[n // 4, pl.ds((n % 4) * 4, 4)].reshape(64, R)
        full = jnp.concatenate([kt, fill_rows[...]], axis=0)
        keys[row, n] = full.T
        return carry

    def kv_copies(h, r):
        for n, ref in enumerate((keys.at[r, pl.ds(h * 4, 4)], values.at[r, h])):
            yield pltpu.make_async_remote_copy(src_ref=ref, dst_ref=ref, send_sem=kv_send.at[h * 2 + n], recv_sem=kv_recv.at[h * 2 + n], device_id=partner, device_id_type=MESH)

    lax.fori_loop(0, 16, project, 0)
    def kv_start(h):
        for copy in kv_copies(h, row):
            copy.start()

    def scatter(h):
        gather.pieces(h, "start")

    gather.forward(0)
    scatter(1)
    lax.fori_loop(0, 16, turn_keys, 0)
    kv_start(0)
    gather.relay(0)
    gather.forward(1)
    scatter(2)
    schedule = (
        (0, kv_start, 1), (1, gather.relay, 1), (1, scatter, 3), (1, kv_start, 2), (2, gather.forward, 2), (2, kv_start, 3),
        (5, gather.relay, 2), (5, gather.forward, 3), (8, gather.relay, 3))

    logits[1] = jnp.zeros((2 * R, 256), F32)
    best[1] = jnp.zeros((1, 256), F32)

    @pl.loop(0, H * NIB)
    def _(n):
        h, ib = n // NIB, n % NIB

        @pl.when(ib == 0)
        def _():
            for copy in kv_copies(h, 1 - row):
                copy.wait_recv()
            gather.finish(h)

        for unit, step, head in schedule:
            pl.when(n == unit)(functools.partial(step, head))

        last = jnp.maximum(n - 1, 0)
        attend(h, ib, (last // NIB, last % NIB), bias_all, query, keys, values, gate, gated, const, bias_kt, logits, best)

    mix(7, H - 1, NIB - 1, values, gate, gated, logits, best)
    project_out(pair_ref, weights, gated, out_ref)

    @pl.loop(0, H)
    def _(h):
        gather.pieces(h, "wait")
        gather.first(h, "wait_send")
        gather.relay(h, "wait_send")
        for copy in kv_copies(h, row):
            copy.wait_send()


def mix(p, h, ib, values, gate, gated, logits, best):
    total = jnp.zeros((1, 256), F32)
    acc = None
    for q in range(4):
        e = jnp.exp2((logits[p % 2, q * 256:q * 256 + 256, :] - best[p % 2]) * LOG2E)
        total = total + jnp.sum(e, axis=0, keepdims=True)
        vs = slice((q % 2) * 256, (q % 2) * 256 + 256)
        v = jnp.concatenate([values[q // 2, h, 2 * p, :, vs], values[q // 2, h, 2 * p + 1, :, vs]], axis=0)
        o = jnp.dot(v, e.astype(BF), preferred_element_type=F32)
        acc = o if acc is None else acc + o
    scale = 1.0 / total
    gated[ib, 2 * p, h] = (gate[h, ib, 2 * p] * (acc[0:16, 0:128] * scale[:, 0:128])).astype(BF)
    gated[ib, 2 * p + 1, h] = (gate[h, ib, 2 * p + 1] * (acc[16:32, 128:256] * scale[:, 128:256])).astype(BF)


def attend(h, ib, before, bias_all, query, keys, values, gate, gated, const, bias_kt, logits, best):
    for t in range(8):
        part = 0 if t < 3 else 1 if t < 6 else 2
        z, y, tile = ib // 2, (ib % 2) * 2, t - PARTS[part][0]
        rows = []
        for n in range(8):
            pos = {"z": z, "y": y + n // 4, "x": n % 4}
            rows.append(bias_all[part][(h, *(pos[dim] for dim in reversed(ORDERS[part])), tile)])
        bias_kt[t * 128:(t + 1) * 128, :] = jnp.concatenate(rows, axis=0).T

    def score(p):
        group, odd = p // 2, p % 2
        zero = jnp.zeros((16, 128), BF)
        gap = jnp.zeros((16, 256), BF)
        left = jnp.concatenate([query[h, ib, 2 * p], zero], axis=1)
        right = jnp.concatenate([zero, query[h, ib, 2 * p + 1]], axis=1)
        top = [gap, gap, left, right] if odd else [left, right, gap, gap]
        rhs = jnp.concatenate(top + [const[...]], axis=0)
        high = None
        for q in range(4):
            rs = slice(q * 256, q * 256 + 256)
            lhs = jnp.concatenate([keys[q // 2, h * 4 + group, (q % 2) * 256:(q % 2) * 256 + 256, :], bias_kt[rs, :]], axis=1)
            s = jnp.dot(lhs, rhs, preferred_element_type=F32)
            logits[p % 2, rs, :] = s
            m = jnp.max(s, axis=0, keepdims=True)
            high = m if high is None else jnp.maximum(high, m)
        best[p % 2] = high

    for p in range(8):
        score(p)
        mix((p + 7) % 8, *((h, ib) if p else before), values, gate, gated, logits, best)


def project_out(pair_ref, weights, gated, out_ref):
    wot = weights[4 * C:5 * C, :]

    def one(j, carry):
        g = jnp.concatenate([gated[ib, j].reshape(64, 128) for ib in range(NIB)], axis=1)
        update = jnp.dot(wot, g, preferred_element_type=F32)
        out_ref[j] = (pair_ref[j].astype(F32) + update).astype(BF)
        return carry

    lax.fori_loop(0, J, one, 0, unroll=8)


SCRATCH = dict(
    normed=((J, C, R), BF), bias_f32=((H, J, R), F32), bias_own=((H, 4, J, 128), BF), spare=((45, J, 128), BF), bias_a=((H, 2, 4, 4, 3, J, 128), BF), bias_b=((H, 4, 2, 4, 3, J, 128), BF), bias_c=((H, 4, 4, 2, 2, J, 128), BF),
    query=((H, NIB, J, D, 128), BF), keys_t=((H, J, D, R), BF), keys=((2, 16, R, 128), BF), values=((2, H, J, D, R), BF),
    gate=((H, NIB, J, D, 128), F32), gated=((NIB, J, H, D, 128), BF), const=((192, 256), BF), fill_rows=((64, R), BF), weights=((5 * C, C), BF),
    bias_kt=((2 * R, 128), BF), logits=((2, 2 * R, 256), F32), best=((2, 1, 256), F32))


def solution(mesh):
    def body(pair_tile, res_mask, ln_gamma, ln_beta, w_q, w_k, w_v, w_b, w_g, w_o):
        pair_t = jnp.transpose(pair_tile, (1, 2, 0))
        scratch = [pltpu.VMEM(shape, dtype) for shape, dtype in SCRATCH.values()]
        sems = [pltpu.SemaphoreType.DMA((n,)) for n in (H * 12, H * 12, H * 3, H * 3, H * 3, 2 * H, 2 * H)]
        out_t = pl.pallas_call(
            kernel,
            out_shape=jax.ShapeDtypeStruct((J, C, R), BF),
            in_specs=[pl.BlockSpec(memory_space=pltpu.VMEM)] * 10,
            out_specs=pl.BlockSpec(memory_space=pltpu.VMEM),
            scratch_shapes=scratch + sems,
            compiler_params=pltpu.CompilerParams(collective_id=0, has_side_effects=True, vmem_limit_bytes=60 * 1024 * 1024),
        )(pair_t, res_mask.reshape(8, 128), ln_gamma.reshape(1, C), ln_beta.reshape(1, C), w_q, w_k, w_v, w_g, w_b.T, w_o)
        return jnp.transpose(out_t, (2, 0, 1))

    tile_spec = P(("data", "row"), "col", None)
    return jax.shard_map(body, mesh=mesh, in_specs=(tile_spec, P("data"), P(), P(), P(), P(), P(), P(), P(), P()), out_specs=tile_spec, check_vma=False)
```

```python
import functools
import math
import jax
import jax.numpy as jnp
from jax import lax
from jax.experimental import pallas as pl
from jax.experimental.pallas import tpu as pltpu
from jax.sharding import PartitionSpec as P

LN_EPS = 1e-5
LOG2E = math.log2(math.e)
FILL_PARTS = (-998244352.0, -1753088.0, -2560.0)
J, C, R, H, D = 16, 64, 512, 4, 16
NIB = 4
MESH = pl.DeviceIdType.MESH
BF, F32 = jnp.bfloat16, jnp.float32
PARTS = ((0, 3), (3, 3), (6, 2))
ORDERS = (("x", "y", "z"), ("y", "z", "x"), ("z", "x", "y"))


class Gather:
    def __init__(self, bias_own, bias_all, spare, send_sem, recv_sem, plane_send, plane_recv, own_send):
        self.own, self.bufs, self.spare, self.send_sem, self.recv_sem = bias_own, bias_all, spare, send_sem, recv_sem
        self.plane_sem, self.plane_recv, self.own_sem = plane_send, plane_recv, own_send
        self.col, self.row = lax.axis_index("col"), lax.axis_index("row")
        self.z, self.y, self.x = self.col // 16, (self.col // 4) % 4, self.col % 4
        self.turn = (self.z - 2 * self.row + 4) % 4
        self.owner = self.z // 2
        self.source = self.turn < 2

    def neighbour(self, dim, step):
        z, y, x = self.z, self.y, self.x
        if dim == "z":
            z = (z + step + 4) % 4
        elif dim == "y":
            y = (y + step + 4) % 4
        else:
            x = (x + step + 4) % 4
        return {"col": (z * 4 + y) * 4 + x, "row": self.row}

    def here(self, dim):
        return {"z": self.z % 2, "y": self.y, "x": self.x}[dim]

    def pieces(self, head, act):
        for r, own in enumerate((((0, 0, 0, 3), (3, 1, 0, 1)), ((0, 1, 1, 2), (2, 2, 0, 2)))):
            for tiles, part, lo, size in own:
                order, sem = ORDERS[part], head * 3 + part
                src = self.own.at[head, pl.ds(tiles, size)]
                dst = self.bufs[part].at[(head, *(self.here(dim) for dim in reversed(order)), pl.ds(lo, size))]

                def away(device, src=src, dst=dst, sem=sem, send=self.plane_sem):
                    return pltpu.make_async_remote_copy(src_ref=src, dst_ref=dst, send_sem=send.at[sem], recv_sem=self.plane_recv.at[sem], device_id=device, device_id_type=MESH)

                def start():
                    @pl.loop(1, 16)
                    def _(n):
                        at = {"z": self.z, "y": self.y, "x": self.x}
                        for dim, step in zip(order[:2], (n % 4, n // 4)):
                            at[dim] = (at[dim] + step) % 4
                        away({"col": (at["z"] * 4 + at["y"]) * 4 + at["x"], "row": self.owner}).start()

                def wait():
                    ref = self.spare.at[pl.ds(0, 15 * size)]
                    away({"row": 1 - self.row}, ref, ref).wait_send()

                def stay():
                    pltpu.make_async_copy(src, dst, self.plane_recv.at[sem]).start()

                def cross():
                    copy = away({"row": 1 - self.row}, send=self.own_sem)
                    copy.start() if act == "start" else copy.wait_send()

                pl.when(self.row == r)(start if act == "start" else wait)
                pl.when((self.row == r) & (self.owner != r))(cross)
                if act == "start":
                    pl.when((self.row == r) & (self.owner == r))(stay)

    def arrived(self, head):
        for part in range(3):
            ref = self.bufs[part].at[head, self.here(ORDERS[part][2])]
            wait = pltpu.make_async_remote_copy(src_ref=ref, dst_ref=ref, send_sem=self.own_sem.at[0], recv_sem=self.plane_recv.at[head * 3 + part], device_id={"row": 1 - self.row}, device_id_type=MESH).wait_recv
            pl.when(self.source)(wait) if part == 0 else wait()

    def copy(self, head, part, slot, value, half, step):
        order = ORDERS[part]
        middle = slice(None)
        if half is not None:
            size = 1 if order[1] == "z" else 2
            middle = pl.ds(half * size, size)
        ref = self.bufs[part].at[head, value, middle]
        sem = (head * 3 + part) * 4 + slot
        return pltpu.make_async_remote_copy(src_ref=ref, dst_ref=ref, send_sem=self.send_sem.at[sem], recv_sem=self.recv_sem.at[sem], device_id=self.neighbour(order[2], step), device_id_type=MESH)

    def first(self, head, act="start"):
        for part in range(3):

            def go():
                for slot, step in ((0, 1), (1, -1)):
                    getattr(self.copy(head, part, slot, self.here(ORDERS[part][2]), None, step), act)()

            pl.when(self.source)(go) if part == 0 else go()

    def relay(self, head, act="start"):
        for part in range(3):
            dim = ORDERS[part][2]
            if dim == "z":
                cases = ((0, 1, 1, 0, -1, 3), (1, 0, 0, 0, 1, 2), (2, 0, 1, 1, 1, 2), (3, 1, 0, 1, -1, 3))
                for turn, slot, value, half, step, out in cases:

                    @pl.when(self.turn == turn)
                    def _():
                        if act == "start":
                            self.copy(head, part, slot, value, None, 1).wait_recv()
                        getattr(self.copy(head, part, out, value, half, step), act)()

                continue
            for slot, back, half, step in ((0, 3, 0, 1), (1, 1, 1, -1)):
                value = (self.here(dim) + back) % 4
                if act == "start":
                    self.copy(head, part, slot, value, None, 1).wait_recv()
                getattr(self.copy(head, part, slot + 2, value, half, step), act)()

    def finish(self, head):
        for part in range(3):
            dim = ORDERS[part][2]
            if dim == "z":
                for turn, value, slots in ((2, 0, ((2, 0), (3, 1))), (3, 1, ((3, 0), (2, 1)))):

                    @pl.when(self.turn == turn)
                    def _():
                        for slot, half in slots:
                            self.copy(head, part, slot, value, half, 1).wait_recv()

                continue
            for slot, half in ((2, 0), (3, 1)):
                self.copy(head, part, slot, (self.here(dim) + 2) % 4, half, 1).wait_recv()

    def forward(self, head):
        self.arrived(head)
        self.first(head)


def kernel(pair_ref, mask_ref, gamma_ref, beta_ref, wq_ref, wk_ref, wv_ref, wg_ref, wbt_ref, wo_ref, out_ref,
           normed, bias_f32, bias_own, spare, bias_a, bias_b, bias_c, query, keys_t, keys, values, gate, gated, const, fill_rows, weights, bias_kt, logits, best,
           send_sem, recv_sem, plane_send, plane_recv, own_send, kv_send, kv_recv):
    row = lax.axis_index("row")
    bias_all = (bias_a, bias_b, bias_c)
    gather = Gather(bias_own, bias_all, spare, send_sem, recv_sem, plane_send, plane_recv, own_send)
    partner = {"row": 1 - row}

    barrier = pltpu.get_barrier_semaphore()
    pl.semaphore_signal(barrier, inc=1, device_id=partner, device_id_type=MESH)

    @pl.loop(1, 64)
    def _(n):
        dz, dy, dx = n // 16, n // 4 % 4, n % 4

        @pl.when((dz == 0) | (dy == 0) | (dx == 0))
        def _():
            col = ((gather.z + dz) % 4 * 4 + (gather.y + dy) % 4) * 4 + (gather.x + dx) % 4
            for r in range(2):
                pl.semaphore_signal(barrier, inc=1, device_id={"col": col, "row": r}, device_id_type=MESH)

    diag = lax.broadcasted_iota(jnp.int32, (C, C), 0) == lax.broadcasted_iota(jnp.int32, (C, C), 1)
    gamma = jnp.sum(jnp.where(diag, gamma_ref[...], 0.0), axis=1, keepdims=True)
    beta = jnp.sum(jnp.where(diag, beta_ref[...], 0.0), axis=1, keepdims=True)
    wbt = wbt_ref[...]
    for j in range(J):
        pair = pair_ref[j].astype(F32)
        mean = jnp.mean(pair, axis=0, keepdims=True)
        centred = pair - mean
        variance = jnp.mean(centred * centred, axis=0, keepdims=True)
        a = (centred * lax.rsqrt(variance + LN_EPS) * gamma + beta).astype(BF)
        normed[j] = a
        b = jnp.dot(wbt, a, preferred_element_type=F32)
        for h in range(H):
            bias_f32[h, j:j + 1, :] = b[h:h + 1, :]
    for h in range(H):
        for t in range(4):
            bias_own[h, t] = bias_f32[h, :, t * 128:(t + 1) * 128].astype(BF)

    pl.semaphore_wait(barrier, 73)

    gather.pieces(0, "start")

    rows_i = lax.broadcasted_iota(jnp.int32, (64, 256), 0)
    const[0:64, :] = jnp.where(rows_i < 3, 1.0, 0.0).astype(BF)
    eye_r = lax.broadcasted_iota(jnp.int32, (128, 256), 0)
    eye_c = lax.broadcasted_iota(jnp.int32, (128, 256), 1)
    const[64:192, :] = jnp.where((eye_c == eye_r) | (eye_c == eye_r + 128), 1.0, 0.0).astype(BF)
    piece = lax.broadcasted_iota(jnp.int32, (64, 128), 0)
    fill = jnp.where(piece == 0, FILL_PARTS[0], jnp.where(piece == 1, FILL_PARTS[1], jnp.where(piece == 2, FILL_PARTS[2], 0.0)))
    for t in range(4):
        shut = jnp.where(mask_ref[pl.ds(row * 4 + t, 1), :] > 0, 0.0, 1.0)
        fill_rows[:, t * 128:(t + 1) * 128] = (fill * shut).astype(BF)
    for n, w_ref in enumerate((wq_ref, wk_ref, wv_ref, wg_ref, wo_ref)):
        weights[n * C:(n + 1) * C, :] = w_ref[...].T
    wt = weights[0:4 * C, :]

    def project(j, carry):
        r = jnp.dot(wt, normed[j], preferred_element_type=F32)
        q = (r[0:64] * (1.0 / math.sqrt(D))).astype(BF)
        k = r[64:128].astype(BF)
        v = r[128:192].astype(BF)
        g = jax.nn.sigmoid(r[192:256])
        for h in range(H):
            sl = slice(h * D, (h + 1) * D)
            keys_t[h, j] = k[sl]
            values[row, h, j] = v[sl]
            for ib in range(NIB):
                query[h, ib, j] = q[sl, ib * 128:(ib + 1) * 128]
                gate[h, ib, j] = g[sl, ib * 128:(ib + 1) * 128]
        return carry

    def turn_keys(n, carry):
        kt = keys_t[n // 4, pl.ds((n % 4) * 4, 4)].reshape(64, R)
        full = jnp.concatenate([kt, fill_rows[...]], axis=0)
        keys[row, n] = full.T
        return carry

    def kv_copies(h, r):
        for n, ref in enumerate((keys.at[r, pl.ds(h * 4, 4)], values.at[r, h])):
            yield pltpu.make_async_remote_copy(src_ref=ref, dst_ref=ref, send_sem=kv_send.at[h * 2 + n], recv_sem=kv_recv.at[h * 2 + n], device_id=partner, device_id_type=MESH)

    lax.fori_loop(0, 16, project, 0, unroll=4)
    def kv_start(h):
        for copy in kv_copies(h, row):
            copy.start()

    def scatter(h):
        gather.pieces(h, "start")

    gather.forward(0)
    scatter(1)
    lax.fori_loop(0, 16, turn_keys, 0, unroll=4)
    kv_start(0)
    gather.relay(0)
    gather.forward(1)
    scatter(2)
    schedule = (
        (0, kv_start, 1), (1, gather.relay, 1), (1, scatter, 3), (1, kv_start, 2), (2, gather.forward, 2), (2, kv_start, 3),
        (5, gather.relay, 2), (5, gather.forward, 3), (8, gather.relay, 3))

    logits[1] = jnp.zeros((2 * R, 256), F32)
    best[1] = jnp.zeros((1, 256), F32)

    @pl.loop(0, H * NIB)
    def _(n):
        h, ib = n // NIB, n % NIB

        @pl.when(ib == 0)
        def _():
            for copy in kv_copies(h, 1 - row):
                copy.wait_recv()
            gather.finish(h)

        for unit, step, head in schedule:
            pl.when(n == unit)(functools.partial(step, head))

        last = jnp.maximum(n - 1, 0)
        attend(h, ib, (last // NIB, last % NIB), bias_all, query, keys, values, gate, gated, const, bias_kt, logits, best)

    mix(7, H - 1, NIB - 1, values, gate, gated, logits, best)
    project_out(pair_ref, weights, gated, out_ref)

    @pl.loop(0, H)
    def _(h):
        gather.pieces(h, "wait")
        gather.first(h, "wait_send")
        gather.relay(h, "wait_send")
        for copy in kv_copies(h, row):
            copy.wait_send()


def mix(p, h, ib, values, gate, gated, logits, best):
    total = jnp.zeros((1, 256), F32)
    acc = None
    for q in range(4):
        e = jnp.exp2((logits[p % 2, q * 256:q * 256 + 256, :] - best[p % 2]) * LOG2E)
        total = total + jnp.sum(e, axis=0, keepdims=True)
        vs = slice((q % 2) * 256, (q % 2) * 256 + 256)
        v = jnp.concatenate([values[q // 2, h, 2 * p, :, vs], values[q // 2, h, 2 * p + 1, :, vs]], axis=0)
        o = jnp.dot(v, e.astype(BF), preferred_element_type=F32)
        acc = o if acc is None else acc + o
    scale = 1.0 / total
    gated[ib, 2 * p, h] = (gate[h, ib, 2 * p] * (acc[0:16, 0:128] * scale[:, 0:128])).astype(BF)
    gated[ib, 2 * p + 1, h] = (gate[h, ib, 2 * p + 1] * (acc[16:32, 128:256] * scale[:, 128:256])).astype(BF)


def attend(h, ib, before, bias_all, query, keys, values, gate, gated, const, bias_kt, logits, best):
    for t in range(8):
        part = 0 if t < 3 else 1 if t < 6 else 2
        z, y, tile = ib // 2, (ib % 2) * 2, t - PARTS[part][0]
        rows = []
        for n in range(8):
            pos = {"z": z, "y": y + n // 4, "x": n % 4}
            rows.append(bias_all[part][(h, *(pos[dim] for dim in reversed(ORDERS[part])), tile)])
        bias_kt[t * 128:(t + 1) * 128, :] = jnp.concatenate(rows, axis=0).T

    def score(p):
        group, odd = p // 2, p % 2
        zero = jnp.zeros((16, 128), BF)
        gap = jnp.zeros((16, 256), BF)
        left = jnp.concatenate([query[h, ib, 2 * p], zero], axis=1)
        right = jnp.concatenate([zero, query[h, ib, 2 * p + 1]], axis=1)
        top = [gap, gap, left, right] if odd else [left, right, gap, gap]
        rhs = jnp.concatenate(top + [const[...]], axis=0)
        high = None
        for q in range(4):
            rs = slice(q * 256, q * 256 + 256)
            lhs = jnp.concatenate([keys[q // 2, h * 4 + group, (q % 2) * 256:(q % 2) * 256 + 256, :], bias_kt[rs, :]], axis=1)
            s = jnp.dot(lhs, rhs, preferred_element_type=F32)
            logits[p % 2, rs, :] = s
            m = jnp.max(s, axis=0, keepdims=True)
            high = m if high is None else jnp.maximum(high, m)
        best[p % 2] = high

    for p in range(8):
        score(p)
        mix((p + 7) % 8, *((h, ib) if p else before), values, gate, gated, logits, best)


def project_out(pair_ref, weights, gated, out_ref):
    wot = weights[4 * C:5 * C, :]

    def one(j, carry):
        g = jnp.concatenate([gated[ib, j].reshape(64, 128) for ib in range(NIB)], axis=1)
        update = jnp.dot(wot, g, preferred_element_type=F32)
        out_ref[j] = (pair_ref[j].astype(F32) + update).astype(BF)
        return carry

    lax.fori_loop(0, J, one, 0, unroll=8)


SCRATCH = dict(
    normed=((J, C, R), BF), bias_f32=((H, J, R), F32), bias_own=((H, 4, J, 128), BF), spare=((45, J, 128), BF), bias_a=((H, 2, 4, 4, 3, J, 128), BF), bias_b=((H, 4, 2, 4, 3, J, 128), BF), bias_c=((H, 4, 4, 2, 2, J, 128), BF),
    query=((H, NIB, J, D, 128), BF), keys_t=((H, J, D, R), BF), keys=((2, 16, R, 128), BF), values=((2, H, J, D, R), BF),
    gate=((H, NIB, J, D, 128), F32), gated=((NIB, J, H, D, 128), BF), const=((192, 256), BF), fill_rows=((64, R), BF), weights=((5 * C, C), BF),
    bias_kt=((2 * R, 128), BF), logits=((2, 2 * R, 256), F32), best=((2, 1, 256), F32))


def solution(mesh):
    def body(pair_tile, res_mask, ln_gamma, ln_beta, w_q, w_k, w_v, w_b, w_g, w_o):
        pair_t = jnp.transpose(pair_tile, (1, 2, 0))
        scratch = [pltpu.VMEM(shape, dtype) for shape, dtype in SCRATCH.values()]
        sems = [pltpu.SemaphoreType.DMA((n,)) for n in (H * 12, H * 12, H * 3, H * 3, H * 3, 2 * H, 2 * H)]
        out_t = pl.pallas_call(
            kernel,
            out_shape=jax.ShapeDtypeStruct((J, C, R), BF),
            in_specs=[pl.BlockSpec(memory_space=pltpu.VMEM)] * 10,
            out_specs=pl.BlockSpec(memory_space=pltpu.VMEM),
            scratch_shapes=scratch + sems,
            compiler_params=pltpu.CompilerParams(collective_id=0, has_side_effects=True, vmem_limit_bytes=60 * 1024 * 1024),
        )(pair_t, res_mask.reshape(8, 128), ln_gamma.reshape(1, C), ln_beta.reshape(1, C), w_q, w_k, w_v, w_g, w_b.T, w_o)
        return jnp.transpose(out_t, (2, 0, 1))

    tile_spec = P(("data", "row"), "col", None)
    return jax.shard_map(body, mesh=mesh, in_specs=(tile_spec, P("data"), P(), P(), P(), P(), P(), P(), P(), P()), out_specs=tile_spec, check_vma=False)
```
